256 devices in a mesh: src: 64 (over x, z, core), grp: 4 (over y).
Axes of the slice: x: 4, y: 4, z: 8, core: 2. Of those that a mesh axis runs over, the one named last changes fastest.
Arguments:
- currents: bfloat16 [524288, 1024], P(('src', 'grp')), may hold values from -6 to 6
- leaf_basis: bfloat16 [2, 40, 524288], P(None, None, ('src', 'grp')), may hold values from -6 to 6
- leaf_box: int32 [524288], P(('src', 'grp')), may hold values from 0 to 7, as said below
- box_count: int32 [2048], P(('src', 'grp')), may hold values from 1 to 2041, as said below
- merge_factor: bfloat16 [2, 2560, 81920], P(None, None, ('src', 'grp')), may hold values from -0.25 to 0.25
- angle_factor: bfloat16 [4096, 4, 2, 2560], P('src'), may hold values from -0.0390625 to 0.0390625
Outputs:
- normalized: float32 [4096, 512], P('src', 'grp')
- peak_value: float32 [512], P('grp')
The draws below stay inside these ranges and needn't reach their ends.
Inputs may be any that keep to these rules, and one draw needn't show every extreme that they name: `leaf_box`: every source block of 2048 currents holds one or more currents of each of its 8 leaf boxes; some blocks put all but 7 of their currents into one box. box_count[k * 8 + b] is the number of currents of source block k whose leaf_box is b.
All inputs are finite; a program needn't handle non-finite values.
Results may differ from the reference program's by a relative error of at most 0.0057.
Values may be sent and summed in bfloat16 or wider, within the bound.
A program may use at most 128 MiB of HBM per device.

```python
import jax
import jax.numpy as jnp
from jax import lax

R = 40
S_DEV = 2048
NE = 512
LEAF = 8
A_DEV = 64
S = 524288
LEAVES = 2048
NA = 4096
N_SRC = 64
N_GRP = 4


def leaf_layout(key):
    blocks = S // S_DEV
    position = jnp.arange(S_DEV, dtype=jnp.int32)[None, :]
    block_ids = jnp.arange(blocks, dtype=jnp.int32)[:, None]
    first_pick = jax.random.randint(jax.random.fold_in(key, 7), (blocks, S_DEV), 0, LEAF)
    second_pick = jax.random.randint(jax.random.fold_in(key, 11), (blocks, S_DEV), 0, LEAF)
    chosen = jnp.minimum(first_pick, second_pick).astype(jnp.int32)
    lone_box = jax.random.randint(jax.random.fold_in(key, 13), (blocks, 1), 0, LEAF).astype(jnp.int32)
    crowded = block_ids % 16 == 0
    chosen = jnp.where(crowded, lone_box, chosen).astype(jnp.int32)
    return jnp.where(position < LEAF, position, chosen).astype(jnp.int32)


def draw_leaf_box(key, part):
    return leaf_layout(key).reshape(S)


def draw_box_count(key, part):
    layout = leaf_layout(key)
    labels = jnp.arange(LEAF, dtype=jnp.int32)
    tallies = jnp.sum((layout[:, None, :] == labels[None, :, None]).astype(jnp.int32), axis=2)
    return tallies.reshape(LEAVES).astype(jnp.int32)


def level_of(rng, shape, pieces, least, largest):
    def one(dim, shards_of):
        draws = jax.random.uniform(jax.random.fold_in(jax.random.fold_in(rng, 6), dim), (shards_of,), jnp.float32, least / len(pieces), largest / len(pieces))
        return jnp.repeat(jnp.exp(draws), shape[dim] // shards_of).reshape((-1,) + (1,) * (len(shape) - dim - 1))

    level = one(*pieces[0])
    for cut in pieces[1:]:
        level = level * one(*cut)
    return level


def centred(own_key, dims, spread, limit, cuts=(), kind=jnp.bfloat16):
    result = spread * jax.random.normal(own_key, dims, jnp.float32)
    if cuts:
        result = result * level_of(own_key, dims, cuts, -0.22, 0.18)
    return jnp.clip(result, -limit, limit).astype(kind)


def setup_inputs(seed: int = 0) -> dict:
    splits = jax.random.split(jax.random.key(seed), 7)
    currents = centred(splits[0], (S, 2 * NE), 1.0, 6.0, ((0, 256),))
    leaf_basis = centred(splits[1], (2, R, S), 1.0, 6.0, ((2, 256),))
    leaf_box = draw_leaf_box(jax.random.fold_in(splits[6], 71), 0)
    box_count = draw_box_count(jax.random.fold_in(splits[6], 71), 0)
    merge_factor = centred(splits[4], (2, N_SRC * R, LEAVES * R), (2 * LEAF * R) ** -0.5, 0.25, ((2, 256),))
    angle_factor = centred(splits[5], (NA, N_GRP, 2, N_SRC * R), (2 * N_SRC * N_GRP * R) ** -0.5, 0.0390625, ((0, 64),))
    return dict(currents=currents, leaf_basis=leaf_basis, leaf_box=leaf_box, box_count=box_count, merge_factor=merge_factor, angle_factor=angle_factor)


def complex_apply(real_part, imag_part, right_side):
    half_width = right_side.shape[1] // 2
    first_part = jnp.dot(real_part, right_side, preferred_element_type=jnp.float32)
    second = jnp.dot(imag_part, right_side, preferred_element_type=jnp.float32)
    return jnp.concatenate([first_part[:, :half_width] - second[:, half_width:], first_part[:, half_width:] + second[:, :half_width]], axis=1)

def source_coefs(currents, leaf_basis, leaf_box, box_count, merge_factor):
    leaf_total = box_count.shape[0]
    rank_size = leaf_basis.shape[1]
    sources = currents.shape[0]
    labels = jnp.arange(leaf_total, dtype=jnp.int32)
    member = (leaf_box[None, :] == labels[:, None]).astype(jnp.float32)
    scaled = member * lax.rsqrt(box_count.astype(jnp.float32))[:, None]
    basis_wide = leaf_basis.astype(jnp.float32)
    left_real = (scaled[:, None, :] * basis_wide[0][None, :, :]).reshape(leaf_total * rank_size, sources).astype(jnp.bfloat16)
    left_imag = (scaled[:, None, :] * basis_wide[1][None, :, :]).reshape(leaf_total * rank_size, sources).astype(jnp.bfloat16)
    leaf_coefs = complex_apply(left_real, left_imag, currents).astype(jnp.bfloat16)
    return complex_apply(merge_factor[0], merge_factor[1], leaf_coefs).astype(jnp.bfloat16)

def angle_side(operands):
    factor, level_coefs = operands
    half_width = level_coefs.shape[2] // 2
    wide_coefs = level_coefs.astype(jnp.float32)
    first_part = jnp.einsum('aqk,qkc->ac', factor[:, :, 0].astype(jnp.float32), wide_coefs)
    second = jnp.einsum('aqk,qkc->ac', factor[:, :, 1].astype(jnp.float32), wide_coefs)
    return jnp.stack([first_part[:, :half_width] - second[:, half_width:], first_part[:, half_width:] + second[:, :half_width]], axis=1)

def reference(currents, leaf_basis, leaf_box, box_count, merge_factor, angle_factor):
    blocks = N_SRC * N_GRP
    rank_size = leaf_basis.shape[1]
    width_cols = currents.shape[1]

    def source_block(block_index):
        first_row = (block_index * S_DEV).astype(jnp.int32)
        first_leaf = (block_index * LEAF).astype(jnp.int32)
        block_currents = lax.dynamic_slice_in_dim(currents, first_row, S_DEV, 0)
        block_basis = lax.dynamic_slice_in_dim(leaf_basis, first_row, S_DEV, 2)
        block_boxes = lax.dynamic_slice_in_dim(leaf_box, first_row, S_DEV, 0)
        block_counts = lax.dynamic_slice_in_dim(box_count, first_leaf, LEAF, 0)
        block_merge = lax.dynamic_slice_in_dim(merge_factor, (first_leaf * rank_size).astype(jnp.int32), LEAF * rank_size, 2)
        return source_coefs(block_currents, block_basis, block_boxes, block_counts, block_merge)
    all_coefs = lax.map(source_block, jnp.arange(blocks, dtype=jnp.int32))
    grouped = all_coefs.reshape(N_SRC, N_GRP, N_SRC, rank_size, width_cols)
    grouped = grouped.transpose(2, 1, 0, 3, 4).reshape(N_SRC, N_GRP, N_SRC * rank_size, width_cols)
    factors = angle_factor.reshape(N_SRC, A_DEV, N_GRP, 2, N_SRC * rank_size)
    patterns = lax.map(angle_side, (factors, grouped))
    pattern = patterns.reshape(N_SRC * A_DEV, 2, width_cols // 2)
    intensity = pattern[:, 0] * pattern[:, 0] + pattern[:, 1] * pattern[:, 1]
    peak_value = lax.optimization_barrier(jnp.max(intensity, axis=0))
    return (intensity / (peak_value[None, :] + 1.0), peak_value)
```

```python
import functools

import jax
import jax.numpy as jnp
from jax import lax
from jax.experimental import pallas as pl
from jax.experimental.pallas import tpu as pltpu
from jax.sharding import PartitionSpec as P

MESH = pl.DeviceIdType.MESH
BF = jnp.bfloat16
F32 = jnp.float32

NX, NY, NZ, NC = 4, 4, 8, 2
CHIPS = NX * NZ
R = 40
LEAF = 8
S_DEV = 2048
NE = 512
A = 64
EQ = NE // NY
LR = LEAF * R
GX = NZ * NC * R


def tdot(a, b):
    return lax.dot_general(a, b, (((0,), (0,)), ((), ())), preferred_element_type=F32)


def dot(a, b):
    return jnp.dot(a, b, preferred_element_type=F32)


def kernel(
    cnt,
    box,
    x_hbm,
    basis_hbm,
    mt_hbm,
    own_hbm,
    inten,
    top_out,
    xv,
    basis,
    mt,
    own,
    ft,
    lmat,
    mm,
    rhs,
    bb,
    rf,
    pa,
    pb,
    ta1,
    tb1,
    ta2,
    tb2,
    ra1,
    rb1,
    ra2,
    rb2,
    qa,
    qb,
    ta3,
    tb3,
    ta4,
    tb4,
    ra3,
    rb3,
    ra4,
    rb4,
    sm,
    rz,
    last32,
    mx,
    m1,
    mz,
    m2,
    ld_sem,
    fs_sem,
    fr_sem,
    ps_sem,
    pr_sem,
    s1,
    r1,
    s2,
    r2,
    zs,
    zr,
    ms,
    mr,
):
    src = lax.axis_index("src")
    y = lax.axis_index("grp")
    c = lax.rem(src, NC)
    z = lax.rem(src // NC, NZ)
    x = src // (NC * NZ)
    chip = src // NC
    mm4 = mm.reshape(NX, NZ, NC * R, 2 * LR)
    ft3 = ft.reshape(CHIPS, NC * R, 2 * A)

    def dev(xx, yy, zz, cc):
        return ((xx * NZ + zz) * NC + cc, yy)

    def remote(a, b, send, recv, to):
        return lambda: pltpu.make_async_remote_copy(
            src_ref=a,
            dst_ref=b,
            send_sem=send,
            recv_sem=recv,
            device_id=to,
            device_id_type=MESH,
        )

    def target_z(k):
        even = (1 - lax.rem(k, 2)) * (k // 2 + 1)
        odd = lax.rem(k, 2) * ((k + 1) // 2 + (k // (NZ - 1)) * (NZ // 2))
        return lax.rem(z + NZ + even - odd, NZ)

    xp, xm, xo = lax.rem(x + 1, NX), lax.rem(x + 3, NX), lax.rem(x + 2, NX)
    yp, ym, yo = lax.rem(y + 1, NY), lax.rem(y + 3, NY), lax.rem(y + 2, NY)
    to_xp, to_xm = dev(xp, y, z, c), dev(xm, y, z, c)
    to_yp, to_ym = dev(x, yp, z, c), dev(x, ym, z, c)
    to_sib = dev(x, y, z, 1 - c)

    loads = [
        pltpu.make_async_copy(a, b, ld_sem.at[i])
        for i, (a, b) in enumerate(
            [(basis_hbm, basis), (mt_hbm, mt), (own_hbm, own), (x_hbm, xv)]
        )
    ]
    for copy in loads:
        copy.start()

    barrier = pltpu.get_barrier_semaphore()

    def greet(i, carry):
        other = lax.rem(chip + i, CHIPS)
        pl.semaphore_signal(
            barrier, inc=1, device_id=(other * NC + c, y), device_id_type=MESH
        )
        return carry

    lax.fori_loop(1, CHIPS, greet, 0)
    greeted = [to_yp, to_ym] + [dev(lax.rem(x + d, NX), y, z, 1 - c) for d in range(NX)]
    for to in greeted:
        pl.semaphore_signal(barrier, inc=1, device_id=to, device_id_type=MESH)

    with jax.named_scope("build"):
        loads[0].wait()
        scale = [
            lax.rsqrt(jnp.full((8, 128), cnt[b], jnp.int32).astype(F32))[0:1, 0:1]
            for b in range(LEAF)
        ]
        width = 256

        def build(i, carry):
            cols = pl.ds(pl.multiple_of(i * width, width), width)
            where = box[:, cols]
            gains = [
                jnp.where(where == b, jnp.broadcast_to(scale[b], (1, width)), 0.0)
                for b in range(LEAF)
            ]
            for p in range(2):
                wide = basis[p, :, cols].astype(F32)
                rows = jnp.concatenate([wide * g for g in gains], axis=0)
                lmat[p * LR : (p + 1) * LR, cols] = rows.astype(BF)
            return carry

        lax.fori_loop(0, S_DEV // width, build, 0)

    with jax.named_scope("turn"):
        loads[1].wait()

        def turn(i, carry):
            span = pl.ds(pl.multiple_of(i * 128, 128), 128)
            mm[span, :] = jnp.transpose(mt[:, span])
            return carry

        lax.fori_loop(0, NX * GX // 128, turn, 0)

    with jax.named_scope("turn_f"):
        loads[2].wait()

        def turn_f(i, carry):
            span = pl.ds(pl.multiple_of(i * 128, 128), 128)
            ft[span, :] = jnp.transpose(own[:, span])
            return carry

        lax.fori_loop(0, NX * GX // 128, turn_f, 0)
        rf[chip] = ft3[chip]

    with jax.named_scope("barrier"):
        pl.semaphore_wait(barrier, CHIPS - 1 + len(greeted))

    def f_copy(i):
        k, dx = i // NX, lax.rem(i, NX)
        tx, tz = lax.rem(x + dx, NX), target_z(k)
        return remote(
            ft3.at[tx * NZ + tz], rf.at[chip], fs_sem.at[i], fr_sem.at[chip], dev(tx, y, tz, c)
        )()

    def f_send(i, carry):
        f_copy(i).start()
        return carry

    with jax.named_scope("f_send"):
        lax.fori_loop(0, CHIPS - NX, f_send, 0)
        lax.fori_loop(CHIPS - NX + 1, CHIPS, f_send, 0)

    tile = 256
    with jax.named_scope("leaf"):
        loads[3].wait()

        def leaf(i, carry):
            lo = pl.ds(pl.multiple_of(i * tile, tile), tile)
            hi = pl.ds(pl.multiple_of(NE + i * tile, tile), tile)
            u = dot(lmat[...], xv[:, lo])
            w = dot(lmat[...], xv[:, hi])
            real = (u[:LR] - w[LR:]).astype(BF)
            imag = (w[:LR] + u[LR:]).astype(BF)
            rhs[:LR, lo] = real
            rhs[LR:, hi] = real
            rhs[:LR, hi] = imag
            rhs[LR:, lo] = -imag
            return carry

        lax.fori_loop(0, NE // tile, leaf, 0)

    def pair_copy(k):
        return remote(bb.at[k, :, 2], bb.at[k, :, c], ps_sem.at[k], pr_sem.at[k], to_sib)()

    def first_copies(k):
        return [
            remote(ta1.at[k, 0:2], ra1.at[k, 0], s1.at[k, 0], r1.at[k, 0], to_xp),
            remote(tb1.at[k, 0:2], rb1.at[k, 0], s1.at[k, 1], r1.at[k, 1], to_yp),
            remote(ta1.at[k, 2:4], ra1.at[k, 1], s1.at[k, 2], r1.at[k, 2], to_xm),
            remote(tb1.at[k, 2:4], rb1.at[k, 1], s1.at[k, 3], r1.at[k, 3], to_ym),
        ]

    def second_copies(k):
        return [
            remote(ta2.at[k, 0], ra2.at[k, 0], s1.at[k, 4], r1.at[k, 4], to_xp),
            remote(tb2.at[k, 0], rb2.at[k, 0], s1.at[k, 5], r1.at[k, 5], to_yp),
            remote(ta2.at[k, 1], ra2.at[k, 1], s1.at[k, 6], r1.at[k, 6], to_xm),
            remote(tb2.at[k, 1], rb2.at[k, 1], s1.at[k, 7], r1.at[k, 7], to_ym),
        ]

    def third_copies(k):
        return [
            remote(ta3.at[k, 0:32], ra3.at[k, 0], s2.at[k, 0], r2.at[k, 0], to_yp),
            remote(tb3.at[k, 0:32], rb3.at[k, 0], s2.at[k, 1], r2.at[k, 1], to_xp),
            remote(ta3.at[k, 32:64], ra3.at[k, 1], s2.at[k, 2], r2.at[k, 2], to_ym),
            remote(tb3.at[k, 32:64], rb3.at[k, 1], s2.at[k, 3], r2.at[k, 3], to_xm),
        ]

    def fourth_copies(k):
        return [
            remote(ta4.at[k, 0], ra4.at[k, 0], s2.at[k, 4], r2.at[k, 4], to_yp),
            remote(tb4.at[k, 0], rb4.at[k, 0], s2.at[k, 5], r2.at[k, 5], to_xp),
            remote(ta4.at[k, 1], ra4.at[k, 1], s2.at[k, 6], r2.at[k, 6], to_ym),
            remote(tb4.at[k, 1], rb4.at[k, 1], s2.at[k, 7], r2.at[k, 7], to_xm),
        ]

    def z_copy(k):
        return remote(sm.at[k], rz.at[k], zs.at[k], zr.at[k], dev(x, y, target_z(k), c))()

    def stage_merge(k):
        left = mm4[:, target_z(k)].reshape(NX * NC * R, 2 * LR)
        for n in range(2 * NE // tile):
            cols = slice(n * tile, (n + 1) * tile)
            v = dot(left, rhs[:, cols])
            for i in range(NX):
                bb[k, i, 2 * c, :, cols] = v[2 * i * R : (2 * i + 1) * R].astype(BF)
                bb[k, i, 2 - c, :, cols] = v[(2 * i + 1) * R : (2 * i + 2) * R].astype(BF)
        pair_copy(k).start()

    def stage_patterns(k):
        tz = target_z(k)

        def arrived(i, carry):
            at = i * NZ + tz

            @pl.when(at != chip)
            def _():
                remote(ft3.at[0], rf.at[at], fs_sem.at[0], fr_sem.at[at], to_sib)().wait_recv()

            return carry

        lax.fori_loop(0, NX, arrived, 0)
        pair_copy(k).wait_recv()
        for i in range(NX):
            q = tdot(rf[i * NZ + tz], bb[k, i, 0:2].reshape(NC * R, 2 * NE))
            real = q[:A, :NE] - q[A:, NE:]
            imag = q[:A, NE:] + q[A:, :NE]
            for j in range(NY):
                pa[k, i, j] = real[:, j * EQ : (j + 1) * EQ]
                pb[k, j, i] = imag[:, j * EQ : (j + 1) * EQ]
        ta1[k] = pa[k, xo].astype(BF)
        tb1[k] = pb[k, yo].astype(BF)
        for copy in first_copies(k):
            copy().start()

    def stage_second(k):
        firsts, seconds = first_copies(k), second_copies(k)
        for n, (p, t, r, to, half) in enumerate(
            [
                (pa, ta2, ra1, xp, 0),
                (pb, tb2, rb1, yp, 0),
                (pa, ta2, ra1, xm, 1),
                (pb, tb2, rb1, ym, 1),
            ]
        ):
            mine, rest = (slice(0, 2), slice(2, 4)) if half == 0 else (slice(2, 4), slice(0, 2))
            t[k, half, rest] = p[k, to, rest].astype(BF)
            firsts[n]().wait_recv()
            t[k, half, mine] = (p[k, to, mine] + r[k, half].astype(F32)).astype(BF)
            seconds[n]().start()

    def stage_third(k):
        seconds, thirds = second_copies(k), third_copies(k)
        for n, (p, q, t, r, me, to) in enumerate(
            [(pa, qa, ta3, ra2, x, yo), (pb, qb, tb3, rb2, y, xo)]
        ):
            seconds[n]().wait_recv()
            seconds[n + 2]().wait_recv()
            q[k] = p[k, me] + r[k, 0].astype(F32) + r[k, 1].astype(F32)
            t[k] = q[k, to].astype(BF)
            thirds[n]().start()
            thirds[n + 2]().start()

    def stage_fourth(k):
        thirds, fourths = third_copies(k), fourth_copies(k)
        for n, (q, t, r, to, half) in enumerate(
            [
                (qa, ta4, ra3, yp, 0),
                (qb, tb4, rb3, xp, 0),
                (qa, ta4, ra3, ym, 1),
                (qb, tb4, rb3, xm, 1),
            ]
        ):
            mine, rest = (slice(0, 32), slice(32, 64)) if half == 0 else (slice(32, 64), slice(0, 32))
            t[k, half, rest] = q[k, to, rest].astype(BF)
            thirds[n]().wait_recv()
            t[k, half, mine] = (q[k, to, mine] + r[k, half].astype(F32)).astype(BF)
            fourths[n]().start()

    def stage_last(k):
        for copy in fourth_copies(k):
            copy().wait_recv()
        real = qa[k, y] + ra4[k, 0].astype(F32) + ra4[k, 1].astype(F32)
        imag = qb[k, x] + rb4[k, 0].astype(F32) + rb4[k, 1].astype(F32)
        last32[0:A] = real
        last32[A:] = imag

        @pl.when(k < NZ - 1)
        def _():
            sm[k, 0:A] = real.astype(BF)
            sm[k, A:] = imag.astype(BF)
            z_copy(k).start()

    stages = [
        (stage_merge, 0),
        (stage_patterns, 1),
        (stage_second, 2),
        (stage_third, 4),
        (stage_fourth, 6),
        (stage_last, 8),
    ]

    def flow(t, carry):
        for stage, lag in stages:

            @pl.when(jnp.logical_and(t >= lag, t < NZ + lag))
            def _(stage=stage, lag=lag):
                with jax.named_scope(stage.__name__):
                    stage(t - lag)

        return carry

    lax.fori_loop(0, NZ + stages[-1][1], flow, 0)

    total = last32[...]
    with jax.named_scope("z_wait"):
        for k in range(NZ - 1):
            z_copy(k).wait_recv()
            total = total + rz[k].astype(F32)
    intensity = total[:A] * total[:A] + total[A:] * total[A:]
    inten[...] = intensity
    mx[...] = jnp.max(intensity, axis=0, keepdims=True)

    slot = x * NC + c
    m1[slot] = mx[...]

    def near(i, sender):
        other = lax.rem(slot + i, NX * NC)
        at = slot if sender else other
        to = dev(other // NC, y, z, lax.rem(other, NC))
        return remote(mx, m1.at[at], ms.at[i], mr.at[at], to)()

    for i in range(1, NX * NC):
        near(i, True).start()
    with jax.named_scope("near_wait"):
        for i in range(1, NX * NC):
            near(i, False).wait_recv()
    mz[...] = jnp.max(m1[...], axis=0)
    m2[z] = mz[...]

    def far(i, sender):
        oz = lax.rem(z + i, NZ)
        at = z if sender else oz
        return remote(mz, m2.at[at], ms.at[NZ + i], mr.at[NZ + at], dev(x, y, oz, c))()

    for i in range(1, NZ):
        far(i, True).start()
    with jax.named_scope("far_wait"):
        for i in range(1, NZ):
            far(i, False).wait_recv()
    top_out[...] = jnp.max(m2[...], axis=0)

    def drain_f(i, carry):
        f_copy(i).wait_send()
        return carry

    def drain(k, carry):
        pair_copy(k).wait_send()
        for copies in (first_copies(k), second_copies(k), third_copies(k), fourth_copies(k)):
            for copy in copies:
                copy().wait_send()

        @pl.when(k < NZ - 1)
        def _():
            z_copy(k).wait_send()
            near(k + 1, True).wait_send()
            far(k + 1, True).wait_send()

        return carry

    with jax.named_scope("drain"):
        lax.fori_loop(0, CHIPS - NX, drain_f, 0)
        lax.fori_loop(CHIPS - NX + 1, CHIPS, drain_f, 0)
        lax.fori_loop(0, NZ, drain, 0)


def finish(inten, top, out, peak):
    peak[...] = top[...]
    out[...] = inten[...] / (top[...] + 1.0)


def body(currents, leaf_basis, leaf_box, box_count, merge_factor, angle_factor):
    own = lax.dynamic_index_in_dim(angle_factor, lax.axis_index("grp"), 1, keepdims=False)
    own = jnp.transpose(own, (1, 0, 2)).reshape(2 * A, NX * GX)
    turned = jnp.transpose(merge_factor, (0, 2, 1)).reshape(2 * LR, NX * GX)

    vm = pltpu.VMEM
    dma = pltpu.SemaphoreType.DMA
    anyspace = pl.BlockSpec(memory_space=pl.ANY)
    invm = pl.BlockSpec(memory_space=pltpu.VMEM)
    shapes = (
        jax.ShapeDtypeStruct((A, EQ), F32),
        jax.ShapeDtypeStruct((1, EQ), F32),
    )
    inten, top = pl.pallas_call(
        kernel,
        out_shape=shapes,
        in_specs=[
            pl.BlockSpec(memory_space=pltpu.SMEM),
            invm,
            anyspace,
            anyspace,
            anyspace,
            anyspace,
        ],
        out_specs=(invm, invm),
        scratch_shapes=[
            vm((S_DEV, 2 * NE), BF),
            vm((2, R, S_DEV), BF),
            vm((2 * LR, NX * GX), BF),
            vm((2 * A, NX * GX), BF),
            vm((NX * GX, 2 * A), BF),
            vm((2 * LR, S_DEV), BF),
            vm((NX * GX, 2 * LR), BF),
            vm((2 * LR, 2 * NE), BF),
            vm((NZ, NX, 3, R, 2 * NE), BF),
            vm((CHIPS, NC * R, 2 * A), BF),
            vm((NZ, NX, NY, A, EQ), F32),
            vm((NZ, NY, NX, A, EQ), F32),
            vm((NZ, 4, A, EQ), BF),
            vm((NZ, 4, A, EQ), BF),
            vm((NZ, 2, 4, A, EQ), BF),
            vm((NZ, 2, 4, A, EQ), BF),
            vm((NZ, 2, 2, A, EQ), BF),
            vm((NZ, 2, 2, A, EQ), BF),
            vm((NZ, 2, 4, A, EQ), BF),
            vm((NZ, 2, 4, A, EQ), BF),
            vm((NZ, NY, A, EQ), F32),
            vm((NZ, NX, A, EQ), F32),
            vm((NZ, A, EQ), BF),
            vm((NZ, A, EQ), BF),
            vm((NZ, 2, A, EQ), BF),
            vm((NZ, 2, A, EQ), BF),
            vm((NZ, 2, A // 2, EQ), BF),
            vm((NZ, 2, A // 2, EQ), BF),
            vm((NZ, 2, A, EQ), BF),
            vm((NZ, 2, A, EQ), BF),
            vm((NZ, 2 * A, EQ), BF),
            vm((NZ, 2 * A, EQ), BF),
            vm((2 * A, EQ), F32),
            vm((1, EQ), F32),
            vm((NX * NC, 1, EQ), F32),
            vm((1, EQ), F32),
            vm((NZ, 1, EQ), F32),
            dma((4,)),
            dma((CHIPS,)),
            dma((CHIPS,)),
            dma((NZ,)),
            dma((NZ,)),
            dma((NZ, 8)),
            dma((NZ, 8)),
            dma((NZ, 8)),
            dma((NZ, 8)),
            dma((NZ,)),
            dma((NZ,)),
            dma((2 * NZ,)),
            dma((2 * NZ,)),
        ],
        compiler_params=pltpu.CompilerParams(
            collective_id=0, has_side_effects=True, vmem_limit_bytes=62 * 1024 * 1024
        ),
    )(
        box_count,
        leaf_box.reshape(1, S_DEV),
        currents,
        leaf_basis,
        turned,
        own,
    )
    normalized, peak = pl.pallas_call(
        finish,
        out_shape=shapes,
        in_specs=[invm, invm],
        out_specs=(invm, invm),
    )(inten, top)
    return normalized, peak.reshape(EQ)


def solution(mesh):
    in_specs = (
        P(("src", "grp"), None),
        P(None, None, ("src", "grp")),
        P(("src", "grp")),
        P(("src", "grp")),
        P(None, None, ("src", "grp")),
        P("src", None, None, None),
    )
    out_specs = (P("src", "grp"), P("grp"))
    return jax.shard_map(body, mesh=mesh, in_specs=in_specs, out_specs=out_specs, check_vma=False)
```

```python
import functools

import jax
import jax.numpy as jnp
from jax import lax
from jax.experimental import pallas as pl
from jax.experimental.pallas import tpu as pltpu
from jax.sharding import PartitionSpec as P

MESH = pl.DeviceIdType.MESH
BF = jnp.bfloat16
F32 = jnp.float32

NX, NY, NZ, NC = 4, 4, 8, 2
CHIPS = NX * NZ
R = 40
LEAF = 8
S_DEV = 2048
NE = 512
A = 64
EQ = NE // NY
LR = LEAF * R
GX = NZ * NC * R
OFFSETS = (1, 7, 2, 6, 4, 3, 5, 0)
LAGS = (0, 1, 3, 6, 8)
AR = 64
BR = 2 * A - AR


def tdot(a, b):
    return lax.dot_general(a, b, (((0,), (0,)), ((), ())), preferred_element_type=F32)


def dot(a, b):
    return jnp.dot(a, b, preferred_element_type=F32)


def kernel(
    cnt,
    box,
    x_hbm,
    basis_hbm,
    mt_hbm,
    own_hbm,
    inten,
    top_out,
    xv,
    basis,
    mt,
    own,
    ft,
    lmat,
    mm,
    rhs,
    bb,
    rf,
    pa,
    pb,
    ta1,
    tb1,
    ta2,
    tb2,
    ra1,
    rb1,
    ra2,
    rb2,
    qa,
    qb,
    sm,
    rz,
    tda,
    tdb,
    rda,
    rdb,
    mx,
    m1,
    mz,
    m2,
    ld_sem,
    fs_sem,
    fr_sem,
    ps_sem,
    pr_sem,
    s1,
    r1,
    zs,
    zr,
    ds,
    dr,
    ms,
    mr,
):
    src = lax.axis_index("src")
    y = lax.axis_index("grp")
    c = lax.rem(src, NC)
    z = lax.rem(src // NC, NZ)
    x = src // (NC * NZ)
    chip = src // NC
    mm4 = mm.reshape(NX, NZ, NC * R, 2 * LR)
    ft3 = ft.reshape(CHIPS, NC * R, 2 * A)

    def dev(xx, yy, zz, cc):
        return ((xx * NZ + zz) * NC + cc, yy)

    def remote(a, b, send, recv, to):
        return lambda: pltpu.make_async_remote_copy(
            src_ref=a,
            dst_ref=b,
            send_sem=send,
            recv_sem=recv,
            device_id=to,
            device_id_type=MESH,
        )

    def target_z(k):
        if isinstance(k, int):
            return lax.rem(z + OFFSETS[k], NZ)
        packed = jnp.int32(sum(o * NZ**i for i, o in enumerate(OFFSETS)))
        return lax.rem(z + lax.rem(lax.shift_right_logical(packed, 3 * k), NZ), NZ)

    xp, xm, xo = lax.rem(x + 1, NX), lax.rem(x + 3, NX), lax.rem(x + 2, NX)
    yp, ym, yo = lax.rem(y + 1, NY), lax.rem(y + 3, NY), lax.rem(y + 2, NY)
    to_xp, to_xm = dev(xp, y, z, c), dev(xm, y, z, c)
    to_yp, to_ym = dev(x, yp, z, c), dev(x, ym, z, c)
    to_sib = dev(x, y, z, 1 - c)

    loads = [
        pltpu.make_async_copy(a, b, ld_sem.at[i])
        for i, (a, b) in enumerate(
            [(own_hbm, own), (basis_hbm, basis), (x_hbm, xv), (mt_hbm, mt)]
        )
    ]
    for copy in loads:
        copy.start()

    barrier = pltpu.get_barrier_semaphore()

    def greet(i, carry):
        other = lax.rem(chip + i, CHIPS)
        pl.semaphore_signal(
            barrier, inc=1, device_id=(other * NC + c, y), device_id_type=MESH
        )
        return carry

    lax.fori_loop(1, CHIPS, greet, 0)
    greeted = [to_yp, to_ym, dev(x, yo, z, c), to_sib]
    for to in greeted:
        pl.semaphore_signal(barrier, inc=1, device_id=to, device_id_type=MESH)

    with jax.named_scope("build"):
        loads[1].wait()
        scale = [
            lax.rsqrt(jnp.full((8, 128), cnt[b], jnp.int32).astype(F32))[0:1, 0:1]
            for b in range(LEAF)
        ]
        width = 256

        def build(i, carry):
            cols = pl.ds(pl.multiple_of(i * width, width), width)
            where = box[:, cols]
            gains = [
                jnp.where(where == b, jnp.broadcast_to(scale[b], (1, width)), 0.0)
                for b in range(LEAF)
            ]
            for p in range(2):
                wide = basis[p, :, cols].astype(F32)
                rows = jnp.concatenate([wide * g for g in gains], axis=0)
                lmat[p * LR : (p + 1) * LR, cols] = rows.astype(BF)
            return carry

        lax.fori_loop(0, S_DEV // width, build, 0)

    with jax.named_scope("turn_f"):
        loads[0].wait()

        for i in range(NX * GX // 128):
            span = slice(i * 128, (i + 1) * 128)
            ft[span, :] = jnp.transpose(own[:, span])
        rf[chip] = ft3[chip]

    with jax.named_scope("barrier"):
        pl.semaphore_wait(barrier, CHIPS - 1 + len(greeted))

    def f_copy(i):
        k, dx = i // NX, i % NX
        tx, tz = lax.rem(x + dx, NX), lax.rem(z + NZ - OFFSETS[k], NZ)
        return remote(
            ft3.at[tx * NZ + tz], rf.at[chip], fs_sem.at[i], fr_sem.at[chip], dev(tx, y, tz, c)
        )()

    with jax.named_scope("f_send"):
        for i in range(CHIPS):
            if i != CHIPS - NX:
                f_copy(i).start()

    tile = 256
    with jax.named_scope("leaf"):
        loads[2].wait()
        loads[3].wait()
        turns = NX * GX // 128 // (NE // tile)

        def leaf(i, carry):
            for n in range(turns):
                span = pl.ds(pl.multiple_of((i * turns + n) * 128, 128), 128)
                mm[span, :] = jnp.transpose(mt[:, span])
            lo = pl.ds(pl.multiple_of(i * tile, tile), tile)
            hi = pl.ds(pl.multiple_of(NE + i * tile, tile), tile)
            u = dot(lmat[...], xv[:, lo])
            w = dot(lmat[...], xv[:, hi])
            real = (u[:LR] - w[LR:]).astype(BF)
            imag = (w[:LR] + u[LR:]).astype(BF)
            rhs[:LR, lo] = real
            rhs[LR:, hi] = real
            rhs[:LR, hi] = imag
            rhs[LR:, lo] = -imag
            return carry

        lax.fori_loop(0, NE // tile, leaf, 0)

    def pair_copy(k):
        return remote(bb.at[k, :, 2], bb.at[k, :, c], ps_sem.at[k], pr_sem.at[k], to_sib)()

    def first_copies(k):
        return [
            remote(ta1.at[k, 0:2], ra1.at[k, 0], s1.at[k, 0], r1.at[k, 0], to_xp),
            remote(tb1.at[k, 0:2], rb1.at[k, 0], s1.at[k, 1], r1.at[k, 1], to_yp),
            remote(ta1.at[k, 2:4], ra1.at[k, 1], s1.at[k, 2], r1.at[k, 2], to_xm),
            remote(tb1.at[k, 2:4], rb1.at[k, 1], s1.at[k, 3], r1.at[k, 3], to_ym),
        ]

    def second_copies(k):
        return [
            remote(ta2.at[k, 0], ra2.at[k, 0], s1.at[k, 4], r1.at[k, 4], to_xp),
            remote(tb2.at[k, 0], rb2.at[k, 0], s1.at[k, 5], r1.at[k, 5], to_yp),
            remote(ta2.at[k, 1], ra2.at[k, 1], s1.at[k, 6], r1.at[k, 6], to_xm),
            remote(tb2.at[k, 1], rb2.at[k, 1], s1.at[k, 7], r1.at[k, 7], to_ym),
        ]

    def direct_copies(k, d, sender):
        oy, ox = lax.rem(y + d, NY), lax.rem(x + d, NX)
        ty, tx = (y, x) if sender else (oy, ox)
        return [
            remote(
                tda.at[k, oy],
                rda.at[k, ty],
                ds.at[k, d],
                dr.at[k, ty],
                dev(x, oy, z, c),
            ),
            remote(
                tdb.at[k, ox],
                rdb.at[k, tx],
                ds.at[k, NY + d],
                dr.at[k, NY + tx],
                dev(ox, y, z, c),
            ),
        ]

    def z_copy(k):
        return remote(sm.at[k], rz.at[k], zs.at[k], zr.at[k], dev(x, y, target_z(k), c))()

    def stage_merge(k):
        left = mm4[:, target_z(k)].reshape(NX * NC * R, 2 * LR)
        for n in range(2 * NE // tile):
            cols = slice(n * tile, (n + 1) * tile)
            v = dot(left, rhs[:, cols])
            for i in range(NX):
                bb[k, i, 2 * c, :, cols] = v[2 * i * R : (2 * i + 1) * R].astype(BF)
                bb[k, i, 2 - c, :, cols] = v[(2 * i + 1) * R : (2 * i + 2) * R].astype(BF)
        pair_copy(k).start()

    def stage_patterns(k):
        tz = target_z(k)

        def arrived(i, carry):
            at = i * NZ + tz

            @pl.when(at != chip)
            def _():
                remote(ft3.at[0], rf.at[at], fs_sem.at[0], fr_sem.at[at], to_sib)().wait_recv()

            return carry

        lax.fori_loop(0, NX, arrived, 0)
        pair_copy(k).wait_recv()
        for i in range(NX):
            q = tdot(rf[i * NZ + tz], bb[k, i, 0:2].reshape(NC * R, 2 * NE))
            real = q[:A, :NE] - q[A:, NE:]
            imag = q[:A, NE:] + q[A:, :NE]
            for j in range(NY):
                pa[k, i, j] = real[:AR, j * EQ : (j + 1) * EQ]
                if AR < A:
                    pb[k, j, i, 0 : A - AR] = real[AR:, j * EQ : (j + 1) * EQ]
                pb[k, j, i, A - AR :] = imag[:, j * EQ : (j + 1) * EQ]
        ta1[k] = pa[k, xo].astype(BF)
        tb1[k] = pb[k, yo].astype(BF)
        for copy in first_copies(k):
            copy().start()

    def stage_second(k):
        firsts, seconds = first_copies(k), second_copies(k)
        for n, (p, t, r, to, half) in enumerate(
            [
                (pa, ta2, ra1, xp, 0),
                (pb, tb2, rb1, yp, 0),
                (pa, ta2, ra1, xm, 1),
                (pb, tb2, rb1, ym, 1),
            ]
        ):
            mine, rest = (slice(0, 2), slice(2, 4)) if half == 0 else (slice(2, 4), slice(0, 2))
            t[k, half, rest] = p[k, to, rest].astype(BF)
            firsts[n]().wait_recv()
            t[k, half, mine] = (p[k, to, mine] + r[k, half].astype(F32)).astype(BF)
            seconds[n]().start()

    def stage_third(k):
        seconds = second_copies(k)
        for n, (p, q, t, r, me) in enumerate([(pa, qa, tda, ra2, x), (pb, qb, tdb, rb2, y)]):
            seconds[n]().wait_recv()
            seconds[n + 2]().wait_recv()
            q[k] = p[k, me] + r[k, 0].astype(F32) + r[k, 1].astype(F32)
            t[k] = q[k].astype(BF)
            for d in (2, 1, 3):
                direct_copies(k, d, True)[n]().start()

    def direct_sum(k):
        one, two = qa[k, y], qb[k, x]
        for d in (1, 3, 2):
            for copy in direct_copies(k, d, False):
                copy().wait_recv()
            one = one + rda[k, lax.rem(y + d, NY)].astype(F32)
            two = two + rdb[k, lax.rem(x + d, NX)].astype(F32)
        return one, two

    def stage_last(k):
        one, two = direct_sum(k)
        sm[k, 0:AR] = one.astype(BF)
        sm[k, AR:] = two.astype(BF)
        z_copy(k).start()

    stages = [
        (stage_merge, LAGS[0], NZ),
        (stage_patterns, LAGS[1], NZ),
        (stage_second, LAGS[2], NZ),
        (stage_third, LAGS[3], NZ),
        (stage_last, LAGS[4], NZ - 1),
    ]

    def flow(t, carry):
        for stage, lag, count in stages:

            @pl.when(jnp.logical_and(t >= lag, t < count + lag))
            def _(stage=stage, lag=lag):
                with jax.named_scope(stage.__name__):
                    stage(t - lag)

        return carry

    lax.fori_loop(0, NZ - 1 + stages[-1][1], flow, 0)

    with jax.named_scope("d_wait"):
        one, two = direct_sum(NZ - 1)
        total = jnp.concatenate([one, two], axis=0)
    with jax.named_scope("z_wait"):
        for k in range(NZ - 1):
            z_copy(k).wait_recv()
            total = total + rz[k].astype(F32)
    intensity = total[:A] * total[:A] + total[A:] * total[A:]
    inten[...] = intensity
    mx[...] = jnp.max(intensity, axis=0, keepdims=True)

    near = remote(mx, m1.at[1], ms.at[0], mr.at[CHIPS], to_sib)()
    near.start()
    with jax.named_scope("near_wait"):
        near.wait_recv()
    mz[...] = jnp.maximum(mx[...], m1[1])
    m2[chip] = mz[...]

    def far(i, sender):
        other = lax.rem(chip + i, CHIPS)
        at = chip if sender else other
        return remote(mz, m2.at[at], ms.at[i], mr.at[at], (other * NC + c, y))()

    def far_send(i, carry):
        far(i, True).start()
        return carry

    def far_wait(i, carry):
        far(i, False).wait_recv()
        return carry

    with jax.named_scope("far_send"):
        lax.fori_loop(1, CHIPS, far_send, 0)
    def drain(k, carry):
        pair_copy(k).wait_send()
        for copies in (first_copies(k), second_copies(k)):
            for copy in copies:
                copy().wait_send()

        for d in range(1, NX):
            for copy in direct_copies(k, d, True):
                copy().wait_send()

        @pl.when(k < NZ - 1)
        def _():
            z_copy(k).wait_send()

        return carry

    def drain_far(i, carry):
        far(i, True).wait_send()
        return carry

    with jax.named_scope("drain"):
        for i in range(CHIPS):
            if i != CHIPS - NX:
                f_copy(i).wait_send()
        lax.fori_loop(0, NZ, drain, 0)
        near.wait_send()

    with jax.named_scope("far_wait"):
        lax.fori_loop(1, CHIPS, far_wait, 0)
    top_out[...] = jnp.max(m2[...], axis=0)
    lax.fori_loop(1, CHIPS, drain_far, 0)


def finish(inten, top, out, peak):
    peak[...] = top[...]
    out[...] = inten[...] / (top[...] + 1.0)


def body(currents, leaf_basis, leaf_box, box_count, merge_factor, angle_factor):
    own = lax.dynamic_index_in_dim(angle_factor, lax.axis_index("grp"), 1, keepdims=False)
    own = jnp.transpose(own, (1, 0, 2)).reshape(2 * A, NX * GX)
    turned = jnp.transpose(merge_factor, (0, 2, 1)).reshape(2 * LR, NX * GX)

    vm = pltpu.VMEM
    dma = pltpu.SemaphoreType.DMA
    anyspace = pl.BlockSpec(memory_space=pl.ANY)
    invm = pl.BlockSpec(memory_space=pltpu.VMEM)
    shapes = (
        jax.ShapeDtypeStruct((A, EQ), F32),
        jax.ShapeDtypeStruct((1, EQ), F32),
    )
    inten, top = pl.pallas_call(
        kernel,
        out_shape=shapes,
        in_specs=[
            pl.BlockSpec(memory_space=pltpu.SMEM),
            invm,
            anyspace,
            anyspace,
            anyspace,
            anyspace,
        ],
        out_specs=(invm, invm),
        scratch_shapes=[
            vm((S_DEV, 2 * NE), BF),
            vm((2, R, S_DEV), BF),
            vm((2 * LR, NX * GX), BF),
            vm((2 * A, NX * GX), BF),
            vm((NX * GX, 2 * A), BF),
            vm((2 * LR, S_DEV), BF),
            vm((NX * GX, 2 * LR), BF),
            vm((2 * LR, 2 * NE), BF),
            vm((NZ, NX, 3, R, 2 * NE), BF),
            vm((CHIPS, NC * R, 2 * A), BF),
            vm((NZ, NX, NY, AR, EQ), F32),
            vm((NZ, NY, NX, BR, EQ), F32),
            vm((NZ, 4, AR, EQ), BF),
            vm((NZ, 4, BR, EQ), BF),
            vm((NZ, 2, 4, AR, EQ), BF),
            vm((NZ, 2, 4, BR, EQ), BF),
            vm((NZ, 2, 2, AR, EQ), BF),
            vm((NZ, 2, 2, BR, EQ), BF),
            vm((NZ, 2, 4, AR, EQ), BF),
            vm((NZ, 2, 4, BR, EQ), BF),
            vm((NZ, NY, AR, EQ), F32),
            vm((NZ, NX, BR, EQ), F32),
            vm((NZ, 2 * A, EQ), BF),
            vm((NZ, 2 * A, EQ), BF),
            vm((NZ, NY, AR, EQ), BF),
            vm((NZ, NX, BR, EQ), BF),
            vm((NZ, NY, AR, EQ), BF),
            vm((NZ, NX, BR, EQ), BF),
            vm((1, EQ), F32),
            vm((2, 1, EQ), F32),
            vm((1, EQ), F32),
            vm((CHIPS, 1, EQ), F32),
            dma((4,)),
            dma((CHIPS,)),
            dma((CHIPS,)),
            dma((NZ,)),
            dma((NZ,)),
            dma((NZ, 8)),
            dma((NZ, 8)),
            dma((NZ,)),
            dma((NZ,)),
            dma((NZ, NX + NY)),
            dma((NZ, NX + NY)),
            dma((CHIPS,)),
            dma((CHIPS + 1,)),
        ],
        compiler_params=pltpu.CompilerParams(
            collective_id=0, has_side_effects=True, vmem_limit_bytes=62 * 1024 * 1024
        ),
    )(
        box_count,
        leaf_box.reshape(1, S_DEV),
        currents,
        leaf_basis,
        turned,
        own,
    )
    normalized, peak = pl.pallas_call(
        finish,
        out_shape=shapes,
        in_specs=[invm, invm],
        out_specs=(invm, invm),
    )(inten, top)
    return normalized, peak.reshape(EQ)


def solution(mesh):
    in_specs = (
        P(("src", "grp"), None),
        P(None, None, ("src", "grp")),
        P(("src", "grp")),
        P(("src", "grp")),
        P(None, None, ("src", "grp")),
        P("src", None, None, None),
    )
    out_specs = (P("src", "grp"), P("grp"))
    return jax.shard_map(body, mesh=mesh, in_specs=in_specs, out_specs=out_specs, check_vma=False)
```

```python
import functools

import jax
import jax.numpy as jnp
from jax import lax
from jax.experimental import pallas as pl
from jax.experimental.pallas import tpu as pltpu
from jax.sharding import PartitionSpec as P

MESH = pl.DeviceIdType.MESH
BF = jnp.bfloat16
F32 = jnp.float32

NX, NY, NZ, NC = 4, 4, 8, 2
CHIPS = NX * NZ
R = 40
LEAF = 8
S_DEV = 2048
NE = 512
A = 64
EQ = NE // NY
LR = LEAF * R
GX = NZ * NC * R
OFFSETS = (1, 7, 2, 5, 3, 4, 6, 0)
LAGS = (0, 1, 3, 6, 9)
AR = 64
BR = 2 * A - AR


def tdot(a, b):
    return lax.dot_general(a, b, (((0,), (0,)), ((), ())), preferred_element_type=F32)


def dot(a, b):
    return jnp.dot(a, b, preferred_element_type=F32)


def kernel(
    cnt_hbm,
    box_hbm,
    x_hbm,
    basis_hbm,
    mt_hbm,
    own_hbm,
    inten_hbm,
    top_out,
    cnt,
    box,
    inten,
    xv,
    basis,
    mt,
    own,
    ft,
    lmat,
    mm,
    rhs,
    bb,
    rf,
    pa,
    pb,
    ta1,
    tb1,
    ta2,
    tb2,
    ra1,
    rb1,
    ra2,
    rb2,
    qa,
    qb,
    sm,
    rz,
    tda,
    tdb,
    rda,
    rdb,
    mx,
    m1,
    mz,
    m2,
    ld_sem,
    fs_sem,
    fr_sem,
    ps_sem,
    pr_sem,
    s1,
    r1,
    zs,
    zr,
    ds,
    dr,
    ms,
    mr,
):
    src = lax.axis_index("src")
    y = lax.axis_index("grp")
    c = lax.rem(src, NC)
    z = lax.rem(src // NC, NZ)
    x = src // (NC * NZ)
    chip = src // NC
    mm4 = mm.reshape(NX, NZ, NC * R, 2 * LR)
    ft3 = ft.reshape(CHIPS, NC * R, 2 * A)

    def dev(xx, yy, zz, cc):
        return ((xx * NZ + zz) * NC + cc, yy)

    def remote(a, b, send, recv, to):
        return lambda: pltpu.make_async_remote_copy(
            src_ref=a,
            dst_ref=b,
            send_sem=send,
            recv_sem=recv,
            device_id=to,
            device_id_type=MESH,
        )

    def target_z(k):
        if isinstance(k, int):
            return lax.rem(z + OFFSETS[k], NZ)
        packed = jnp.int32(sum(o * NZ**i for i, o in enumerate(OFFSETS)))
        return lax.rem(z + lax.rem(lax.shift_right_logical(packed, 3 * k), NZ), NZ)

    xp, xm, xo = lax.rem(x + 1, NX), lax.rem(x + 3, NX), lax.rem(x + 2, NX)
    yp, ym, yo = lax.rem(y + 1, NY), lax.rem(y + 3, NY), lax.rem(y + 2, NY)
    to_xp, to_xm = dev(xp, y, z, c), dev(xm, y, z, c)
    to_yp, to_ym = dev(x, yp, z, c), dev(x, ym, z, c)
    to_sib = dev(x, y, z, 1 - c)

    loads = [
        pltpu.make_async_copy(a, b, ld_sem.at[i])
        for i, (a, b) in enumerate(
            [
                (own_hbm.at[:, y], own),
                (cnt_hbm, cnt),
                (box_hbm, box),
                (basis_hbm, basis),
                (x_hbm, xv),
                (mt_hbm, mt),
            ]
        )
    ]
    for copy in loads:
        copy.start()

    barrier = pltpu.get_barrier_semaphore()

    def greet(i, carry):
        other = lax.rem(chip + i, CHIPS)
        pl.semaphore_signal(
            barrier, inc=1, device_id=(other * NC + c, y), device_id_type=MESH
        )
        return carry

    lax.fori_loop(1, CHIPS, greet, 0)
    greeted = [to_yp, to_ym, dev(x, yo, z, c), to_sib]
    for to in greeted:
        pl.semaphore_signal(barrier, inc=1, device_id=to, device_id_type=MESH)

    with jax.named_scope("turn_f"):
        loads[0].wait()

        for i in range(NX * GX // 128):
            span = slice(i * 128, (i + 1) * 128)
            pair = own[:, :, span]
            both = jnp.concatenate([pair[:, 0, :], pair[:, 1, :]], axis=0)
            ft[span, :] = jnp.transpose(both)
        rf[chip] = ft3[chip]

    with jax.named_scope("build"):
        for copy in loads[1:4]:
            copy.wait()
        scale = [
            lax.rsqrt(jnp.full((8, 128), cnt[b], jnp.int32).astype(F32))[0:1, 0:1]
            for b in range(LEAF)
        ]
        width = 256

        def build(i, carry):
            cols = pl.ds(pl.multiple_of(i * width, width), width)
            where = box[:, cols]
            gains = [
                jnp.where(where == b, jnp.broadcast_to(scale[b], (1, width)), 0.0)
                for b in range(LEAF)
            ]
            for p in range(2):
                wide = basis[p, :, cols].astype(F32)
                rows = jnp.concatenate([wide * g for g in gains], axis=0)
                lmat[p * LR : (p + 1) * LR, cols] = rows.astype(BF)
            return carry

        lax.fori_loop(0, S_DEV // width, build, 0)

    with jax.named_scope("barrier"):
        pl.semaphore_wait(barrier, CHIPS - 1 + len(greeted))

    def f_copy(i):
        k, dx = i // NX, i % NX
        tx, tz = lax.rem(x + dx, NX), lax.rem(z + NZ - OFFSETS[k], NZ)
        return remote(
            ft3.at[tx * NZ + tz], rf.at[chip], fs_sem.at[i], fr_sem.at[chip], dev(tx, y, tz, c)
        )()

    with jax.named_scope("f_send"):
        for i in range(CHIPS):
            if i != CHIPS - NX:
                f_copy(i).start()

    tile = 256
    with jax.named_scope("leaf"):
        loads[4].wait()
        loads[5].wait()
        turns = NX * GX // 128 // (NE // tile)

        def leaf(i, carry):
            for n in range(turns):
                span = pl.ds(pl.multiple_of((i * turns + n) * 128, 128), 128)
                mm[span, :] = jnp.transpose(mt[:, span])
            lo = pl.ds(pl.multiple_of(i * tile, tile), tile)
            hi = pl.ds(pl.multiple_of(NE + i * tile, tile), tile)
            u = dot(lmat[...], xv[:, lo])
            w = dot(lmat[...], xv[:, hi])
            real = (u[:LR] - w[LR:]).astype(BF)
            imag = (w[:LR] + u[LR:]).astype(BF)
            rhs[:LR, lo] = real
            rhs[LR:, hi] = real
            rhs[:LR, hi] = imag
            rhs[LR:, lo] = -imag
            return carry

        lax.fori_loop(0, NE // tile, leaf, 0)

    def pair_copy(k):
        return remote(bb.at[k, :, 2], bb.at[k, :, c], ps_sem.at[k], pr_sem.at[k], to_sib)()

    def first_copies(k):
        return [
            remote(ta1.at[k, 0:2], ra1.at[k, 0], s1.at[k, 0], r1.at[k, 0], to_xp),
            remote(tb1.at[k, 0:2], rb1.at[k, 0], s1.at[k, 1], r1.at[k, 1], to_yp),
            remote(ta1.at[k, 2:4], ra1.at[k, 1], s1.at[k, 2], r1.at[k, 2], to_xm),
            remote(tb1.at[k, 2:4], rb1.at[k, 1], s1.at[k, 3], r1.at[k, 3], to_ym),
        ]

    def second_copies(k):
        return [
            remote(ta2.at[k, 0], ra2.at[k, 0], s1.at[k, 4], r1.at[k, 4], to_xp),
            remote(tb2.at[k, 0], rb2.at[k, 0], s1.at[k, 5], r1.at[k, 5], to_yp),
            remote(ta2.at[k, 1], ra2.at[k, 1], s1.at[k, 6], r1.at[k, 6], to_xm),
            remote(tb2.at[k, 1], rb2.at[k, 1], s1.at[k, 7], r1.at[k, 7], to_ym),
        ]

    def direct_copies(k, d, sender):
        oy, ox = lax.rem(y + d, NY), lax.rem(x + d, NX)
        ty, tx = (y, x) if sender else (oy, ox)
        return [
            remote(
                tda.at[k, oy],
                rda.at[k, ty],
                ds.at[k, d],
                dr.at[k, ty],
                dev(x, oy, z, c),
            ),
            remote(
                tdb.at[k, ox],
                rdb.at[k, tx],
                ds.at[k, NY + d],
                dr.at[k, NY + tx],
                dev(ox, y, z, c),
            ),
        ]

    def z_copy(k):
        return remote(sm.at[k], rz.at[k], zs.at[k], zr.at[k], dev(x, y, target_z(k), c))()

    def stage_merge(k):
        left = mm4[:, target_z(k)].reshape(NX * NC * R, 2 * LR)
        for n in range(2 * NE // tile):
            cols = slice(n * tile, (n + 1) * tile)
            v = dot(left, rhs[:, cols])
            for i in range(NX):
                bb[k, i, 2 * c, :, cols] = v[2 * i * R : (2 * i + 1) * R].astype(BF)
                bb[k, i, 2 - c, :, cols] = v[(2 * i + 1) * R : (2 * i + 2) * R].astype(BF)
        pair_copy(k).start()

    def stage_patterns(k):
        tz = target_z(k)

        def arrived(i, carry):
            at = i * NZ + tz

            @pl.when(at != chip)
            def _():
                remote(ft3.at[0], rf.at[at], fs_sem.at[0], fr_sem.at[at], to_sib)().wait_recv()

            return carry

        lax.fori_loop(0, NX, arrived, 0)
        pair_copy(k).wait_recv()
        for i in range(NX):
            q = tdot(rf[i * NZ + tz], bb[k, i, 0:2].reshape(NC * R, 2 * NE))
            real = q[:A, :NE] - q[A:, NE:]
            imag = q[:A, NE:] + q[A:, :NE]
            for j in range(NY):
                pa[k, i, j] = real[:AR, j * EQ : (j + 1) * EQ]
                if AR < A:
                    pb[k, j, i, 0 : A - AR] = real[AR:, j * EQ : (j + 1) * EQ]
                pb[k, j, i, A - AR :] = imag[:, j * EQ : (j + 1) * EQ]
        ta1[k] = pa[k, xo].astype(BF)
        tb1[k] = pb[k, yo].astype(BF)
        for copy in first_copies(k):
            copy().start()

    def stage_second(k):
        firsts, seconds = first_copies(k), second_copies(k)
        for n, (p, t, r, to, half) in enumerate(
            [
                (pa, ta2, ra1, xp, 0),
                (pb, tb2, rb1, yp, 0),
                (pa, ta2, ra1, xm, 1),
                (pb, tb2, rb1, ym, 1),
            ]
        ):
            mine, rest = (slice(0, 2), slice(2, 4)) if half == 0 else (slice(2, 4), slice(0, 2))
            t[k, half, rest] = p[k, to, rest].astype(BF)
            firsts[n]().wait_recv()
            t[k, half, mine] = (p[k, to, mine] + r[k, half].astype(F32)).astype(BF)
            seconds[n]().start()

    def stage_third(k):
        seconds = second_copies(k)
        for n, (p, q, t, r, me) in enumerate([(pa, qa, tda, ra2, x), (pb, qb, tdb, rb2, y)]):
            seconds[n]().wait_recv()
            seconds[n + 2]().wait_recv()
            q[k] = p[k, me] + r[k, 0].astype(F32) + r[k, 1].astype(F32)
            t[k] = q[k].astype(BF)
            for d in (2, 1, 3):
                direct_copies(k, d, True)[n]().start()

    def direct_sum(k):
        one, two = qa[k, y], qb[k, x]
        for d in (1, 3, 2):
            for copy in direct_copies(k, d, False):
                copy().wait_recv()
            one = one + rda[k, lax.rem(y + d, NY)].astype(F32)
            two = two + rdb[k, lax.rem(x + d, NX)].astype(F32)
        return one, two

    def stage_last(k):
        one, two = direct_sum(k)
        sm[k, 0:AR] = one.astype(BF)
        sm[k, AR:] = two.astype(BF)
        z_copy(k).start()

    stages = [
        (stage_merge, LAGS[0], NZ),
        (stage_second, LAGS[2], NZ),
        (stage_third, LAGS[3], NZ),
        (stage_patterns, LAGS[1], NZ),
        (stage_last, LAGS[4], NZ - 1),
    ]

    def flow(t, carry):
        for stage, lag, count in stages:

            @pl.when(jnp.logical_and(t >= lag, t < count + lag))
            def _(stage=stage, lag=lag):
                with jax.named_scope(stage.__name__):
                    stage(t - lag)

        return carry

    lax.fori_loop(0, NZ - 1 + stages[-1][1], flow, 0)

    with jax.named_scope("d_wait"):
        one, two = direct_sum(NZ - 1)
        total = jnp.concatenate([one, two], axis=0)
    with jax.named_scope("z_wait"):
        for k in range(NZ - 1):
            z_copy(k).wait_recv()
            total = total + rz[k].astype(F32)
    intensity = total[:A] * total[:A] + total[A:] * total[A:]
    inten[...] = intensity
    save = pltpu.make_async_copy(inten, inten_hbm, ld_sem.at[6])
    save.start()
    mx[...] = jnp.max(intensity, axis=0, keepdims=True)

    near = remote(mx, m1.at[1], ms.at[0], mr.at[CHIPS], to_sib)()
    near.start()
    with jax.named_scope("near_wait"):
        near.wait_recv()
    mz[...] = jnp.maximum(mx[...], m1[1])
    m2[chip] = mz[...]

    def far(i, sender):
        other = lax.rem(chip + i, CHIPS)
        at = chip if sender else other
        return remote(mz, m2.at[at], ms.at[i], mr.at[at], (other * NC + c, y))()

    def far_send(i, carry):
        far(i, True).start()
        return carry

    def far_wait(i, carry):
        far(i, False).wait_recv()
        return carry

    with jax.named_scope("far_send"):
        lax.fori_loop(1, CHIPS, far_send, 0)
    def drain(k, carry):
        pair_copy(k).wait_send()
        for copies in (first_copies(k), second_copies(k)):
            for copy in copies:
                copy().wait_send()

        for d in range(1, NX):
            for copy in direct_copies(k, d, True):
                copy().wait_send()

        @pl.when(k < NZ - 1)
        def _():
            z_copy(k).wait_send()

        return carry

    def drain_far(i, carry):
        far(i, True).wait_send()
        return carry

    with jax.named_scope("drain"):
        for i in range(CHIPS):
            if i != CHIPS - NX:
                f_copy(i).wait_send()
        lax.fori_loop(0, NZ, drain, 0)
        near.wait_send()

    with jax.named_scope("far_wait"):
        lax.fori_loop(1, CHIPS, far_wait, 0)
    top_out[...] = jnp.max(m2[...], axis=0)
    lax.fori_loop(1, CHIPS, drain_far, 0)
    save.wait()


def finish(inten, top, out, peak):
    peak[...] = top[...]
    out[...] = inten[...] / (top[...] + 1.0)


def body(currents, leaf_basis, leaf_box, box_count, merge_factor, angle_factor):
    turned = jnp.transpose(merge_factor, (0, 2, 1)).reshape(2 * LR, NX * GX)

    vm = pltpu.VMEM
    dma = pltpu.SemaphoreType.DMA
    anyspace = pl.BlockSpec(memory_space=pl.ANY)
    invm = pl.BlockSpec(memory_space=pltpu.VMEM)
    shapes = (
        jax.ShapeDtypeStruct((A, EQ), F32),
        jax.ShapeDtypeStruct((1, EQ), F32),
    )
    inten, top = pl.pallas_call(
        kernel,
        out_shape=shapes,
        in_specs=[anyspace] * 6,
        out_specs=(anyspace, invm),
        scratch_shapes=[
            pltpu.SMEM((LEAF,), jnp.int32),
            vm((1, S_DEV), jnp.int32),
            vm((A, EQ), F32),
            vm((S_DEV, 2 * NE), BF),
            vm((2, R, S_DEV), BF),
            vm((2 * LR, NX * GX), BF),
            vm((A, 2, NX * GX), BF),
            vm((NX * GX, 2 * A), BF),
            vm((2 * LR, S_DEV), BF),
            vm((NX * GX, 2 * LR), BF),
            vm((2 * LR, 2 * NE), BF),
            vm((NZ, NX, 3, R, 2 * NE), BF),
            vm((CHIPS, NC * R, 2 * A), BF),
            vm((NZ, NX, NY, AR, EQ), F32),
            vm((NZ, NY, NX, BR, EQ), F32),
            vm((NZ, 4, AR, EQ), BF),
            vm((NZ, 4, BR, EQ), BF),
            vm((NZ, 2, 4, AR, EQ), BF),
            vm((NZ, 2, 4, BR, EQ), BF),
            vm((NZ, 2, 2, AR, EQ), BF),
            vm((NZ, 2, 2, BR, EQ), BF),
            vm((NZ, 2, 4, AR, EQ), BF),
            vm((NZ, 2, 4, BR, EQ), BF),
            vm((NZ, NY, AR, EQ), F32),
            vm((NZ, NX, BR, EQ), F32),
            vm((NZ, 2 * A, EQ), BF),
            vm((NZ, 2 * A, EQ), BF),
            vm((NZ, NY, AR, EQ), BF),
            vm((NZ, NX, BR, EQ), BF),
            vm((NZ, NY, AR, EQ), BF),
            vm((NZ, NX, BR, EQ), BF),
            vm((1, EQ), F32),
            vm((2, 1, EQ), F32),
            vm((1, EQ), F32),
            vm((CHIPS, 1, EQ), F32),
            dma((7,)),
            dma((CHIPS,)),
            dma((CHIPS,)),
            dma((NZ,)),
            dma((NZ,)),
            dma((NZ, 8)),
            dma((NZ, 8)),
            dma((NZ,)),
            dma((NZ,)),
            dma((NZ, NX + NY)),
            dma((NZ, NX + NY)),
            dma((CHIPS,)),
            dma((CHIPS + 1,)),
        ],
        compiler_params=pltpu.CompilerParams(
            collective_id=0, has_side_effects=True, vmem_limit_bytes=62 * 1024 * 1024
        ),
    )(
        box_count,
        leaf_box.reshape(1, S_DEV),
        currents,
        leaf_basis,
        turned,
        angle_factor,
    )
    normalized, peak = pl.pallas_call(
        finish,
        out_shape=shapes,
        in_specs=[invm, invm],
        out_specs=(invm, invm),
    )(inten, top)
    return normalized, peak.reshape(EQ)


def solution(mesh):
    in_specs = (
        P(("src", "grp"), None),
        P(None, None, ("src", "grp")),
        P(("src", "grp")),
        P(("src", "grp")),
        P(None, None, ("src", "grp")),
        P("src", None, None, None),
    )
    out_specs = (P("src", "grp"), P("grp"))
    return jax.shard_map(body, mesh=mesh, in_specs=in_specs, out_specs=out_specs, check_vma=False)
```

```python
import functools

import jax
import jax.numpy as jnp
from jax import lax
from jax.experimental import pallas as pl
from jax.experimental.pallas import tpu as pltpu
from jax.sharding import PartitionSpec as P

MESH = pl.DeviceIdType.MESH
BF = jnp.bfloat16
F32 = jnp.float32

NX, NY, NZ, NC = 4, 4, 8, 2
CHIPS = NX * NZ
R = 40
LEAF = 8
S_DEV = 2048
NE = 512
A = 64
EQ = NE // NY
LR = LEAF * R
GX = NZ * NC * R
OFFSETS = (1, 7, 2, 5, 3, 4, 6, 0)
LAGS = (0, 1, 4, 7, 10)
AR = 64
BR = 2 * A - AR
RAW = 4


def tdot(a, b):
    return lax.dot_general(a, b, (((0,), (0,)), ((), ())), preferred_element_type=F32)


def dot(a, b):
    return jnp.dot(a, b, preferred_element_type=F32)


def kernel(
    cnt_hbm,
    box_hbm,
    x_hbm,
    basis_hbm,
    mt_hbm,
    own_hbm,
    inten_hbm,
    top_out,
    cnt,
    box,
    inten,
    xv,
    basis,
    mt,
    own,
    ft,
    lmat,
    mm,
    rhs,
    bb,
    rf,
    pa,
    pb,
    ta1,
    tb1,
    ta2,
    tb2,
    ra1,
    rb1,
    ra2,
    rb2,
    qa,
    qb,
    sm,
    rz,
    wa,
    wb,
    va,
    vb,
    tda,
    tdb,
    rda,
    rdb,
    mx,
    m1,
    mz,
    m2,
    ld_sem,
    fs_sem,
    fr_sem,
    ps_sem,
    pr_sem,
    s1,
    r1,
    zs,
    zr,
    ds,
    dr,
    ws,
    wr,
    ms,
    mr,
):
    src = lax.axis_index("src")
    y = lax.axis_index("grp")
    c = lax.rem(src, NC)
    z = lax.rem(src // NC, NZ)
    x = src // (NC * NZ)
    chip = src // NC
    mm4 = mm.reshape(NX, NZ, NC * R, 2 * LR)
    ft3 = ft.reshape(CHIPS, NC * R, 2 * A)

    def dev(xx, yy, zz, cc):
        return ((xx * NZ + zz) * NC + cc, yy)

    def remote(a, b, send, recv, to):
        return lambda: pltpu.make_async_remote_copy(
            src_ref=a,
            dst_ref=b,
            send_sem=send,
            recv_sem=recv,
            device_id=to,
            device_id_type=MESH,
        )

    def target_z(k):
        if isinstance(k, int):
            return lax.rem(z + OFFSETS[k], NZ)
        packed = jnp.int32(sum(o * NZ**i for i, o in enumerate(OFFSETS)))
        return lax.rem(z + lax.rem(lax.shift_right_logical(packed, 3 * k), NZ), NZ)

    xp, xm, xo = lax.rem(x + 1, NX), lax.rem(x + 3, NX), lax.rem(x + 2, NX)
    yp, ym, yo = lax.rem(y + 1, NY), lax.rem(y + 3, NY), lax.rem(y + 2, NY)
    to_xp, to_xm = dev(xp, y, z, c), dev(xm, y, z, c)
    to_yp, to_ym = dev(x, yp, z, c), dev(x, ym, z, c)
    to_sib = dev(x, y, z, 1 - c)

    loads = [
        pltpu.make_async_copy(a, b, ld_sem.at[i])
        for i, (a, b) in enumerate(
            [
                (own_hbm.at[:, y], own),
                (cnt_hbm, cnt),
                (box_hbm, box),
                (basis_hbm, basis),
                (x_hbm, xv),
                (mt_hbm, mt),
            ]
        )
    ]
    for copy in loads:
        copy.start()

    barrier = pltpu.get_barrier_semaphore()

    def greet(i, carry):
        other = lax.rem(chip + i, CHIPS)
        pl.semaphore_signal(
            barrier, inc=1, device_id=(other * NC + c, y), device_id_type=MESH
        )
        return carry

    lax.fori_loop(1, CHIPS, greet, 0)
    greeted = [to_yp, to_ym, dev(x, yo, z, c), to_sib]
    for to in greeted:
        pl.semaphore_signal(barrier, inc=1, device_id=to, device_id_type=MESH)

    with jax.named_scope("turn_f"):
        loads[0].wait()

        for i in range(NX * GX // 128):
            span = slice(i * 128, (i + 1) * 128)
            pair = own[:, :, span]
            both = jnp.concatenate([pair[:, 0, :], pair[:, 1, :]], axis=0)
            ft[span, :] = jnp.transpose(both)
        rf[chip] = ft3[chip]

    with jax.named_scope("build"):
        for copy in loads[1:4]:
            copy.wait()
        scale = [
            lax.rsqrt(jnp.full((8, 128), cnt[b], jnp.int32).astype(F32))[0:1, 0:1]
            for b in range(LEAF)
        ]
        width = 256

        def build(i, carry):
            cols = pl.ds(pl.multiple_of(i * width, width), width)
            where = box[:, cols]
            gains = [
                jnp.where(where == b, jnp.broadcast_to(scale[b], (1, width)), 0.0)
                for b in range(LEAF)
            ]
            for p in range(2):
                wide = basis[p, :, cols].astype(F32)
                rows = jnp.concatenate([wide * g for g in gains], axis=0)
                lmat[p * LR : (p + 1) * LR, cols] = rows.astype(BF)
            return carry

        lax.fori_loop(0, S_DEV // width, build, 0)

    with jax.named_scope("barrier"):
        pl.semaphore_wait(barrier, CHIPS - 1 + len(greeted))

    def f_copy(i):
        k, dx = i // NX, i % NX
        tx, tz = lax.rem(x + dx, NX), lax.rem(z + NZ - OFFSETS[k], NZ)
        return remote(
            ft3.at[tx * NZ + tz], rf.at[chip], fs_sem.at[i], fr_sem.at[chip], dev(tx, y, tz, c)
        )()

    with jax.named_scope("f_send"):
        for i in range(CHIPS):
            if i != CHIPS - NX:
                f_copy(i).start()

    tile = 256
    with jax.named_scope("leaf"):
        loads[4].wait()
        loads[5].wait()
        turns = NX * GX // 128 // (NE // tile)

        def leaf(i, carry):
            for n in range(turns):
                span = pl.ds(pl.multiple_of((i * turns + n) * 128, 128), 128)
                mm[span, :] = jnp.transpose(mt[:, span])
            lo = pl.ds(pl.multiple_of(i * tile, tile), tile)
            hi = pl.ds(pl.multiple_of(NE + i * tile, tile), tile)
            u = dot(lmat[...], xv[:, lo])
            w = dot(lmat[...], xv[:, hi])
            real = (u[:LR] - w[LR:]).astype(BF)
            imag = (w[:LR] + u[LR:]).astype(BF)
            rhs[:LR, lo] = real
            rhs[LR:, hi] = real
            rhs[:LR, hi] = imag
            rhs[LR:, lo] = -imag
            return carry

        lax.fori_loop(0, NE // tile, leaf, 0)

    def pair_copy(k):
        return remote(bb.at[k, :, 2], bb.at[k, :, c], ps_sem.at[k], pr_sem.at[k], to_sib)()

    def first_copies(k):
        return [
            remote(ta1.at[k, 0:2], ra1.at[k, 0], s1.at[k, 0], r1.at[k, 0], to_xp),
            remote(tb1.at[k, 0:2], rb1.at[k, 0], s1.at[k, 1], r1.at[k, 1], to_yp),
            remote(ta1.at[k, 2:4], ra1.at[k, 1], s1.at[k, 2], r1.at[k, 2], to_xm),
            remote(tb1.at[k, 2:4], rb1.at[k, 1], s1.at[k, 3], r1.at[k, 3], to_ym),
        ]

    def second_copies(k):
        return [
            remote(ta2.at[k, 0], ra2.at[k, 0], s1.at[k, 4], r1.at[k, 4], to_xp),
            remote(tb2.at[k, 0], rb2.at[k, 0], s1.at[k, 5], r1.at[k, 5], to_yp),
            remote(ta2.at[k, 1], ra2.at[k, 1], s1.at[k, 6], r1.at[k, 6], to_xm),
            remote(tb2.at[k, 1], rb2.at[k, 1], s1.at[k, 7], r1.at[k, 7], to_ym),
        ]

    def direct_copies(k, d, sender):
        oy, ox = lax.rem(y + d, NY), lax.rem(x + d, NX)
        ty, tx = (y, x) if sender else (oy, ox)
        return [
            remote(
                tda.at[k, oy],
                rda.at[k, ty],
                ds.at[k, d],
                dr.at[k, ty],
                dev(x, oy, z, c),
            ),
            remote(
                tdb.at[k, ox],
                rdb.at[k, tx],
                ds.at[k, NY + d],
                dr.at[k, NY + tx],
                dev(ox, y, z, c),
            ),
        ]

    def raw_copies():
        up, down = lax.rem(z + 1, NZ), lax.rem(z + NZ - 1, NZ)
        return [
            remote(wa, va, ws.at[0], wr.at[0], dev(x, y, up, c)),
            remote(wb, vb, ws.at[1], wr.at[1], dev(x, y, down, c)),
        ]

    def z_copy(k):
        return remote(sm.at[k], rz.at[k], zs.at[k], zr.at[k], dev(x, y, target_z(k), c))()

    def stage_merge(k):
        left = mm4[:, target_z(k)].reshape(NX * NC * R, 2 * LR)
        for n in range(2 * NE // tile):
            cols = slice(n * tile, (n + 1) * tile)
            v = dot(left, rhs[:, cols])
            for i in range(NX):
                bb[k, i, 2 * c, :, cols] = v[2 * i * R : (2 * i + 1) * R].astype(BF)
                bb[k, i, 2 - c, :, cols] = v[(2 * i + 1) * R : (2 * i + 2) * R].astype(BF)
        pair_copy(k).start()

    def stage_patterns(k):
        tz = target_z(k)

        def arrived(i, carry):
            at = i * NZ + tz

            @pl.when(at != chip)
            def _():
                remote(ft3.at[0], rf.at[at], fs_sem.at[0], fr_sem.at[at], to_sib)().wait_recv()

            return carry

        lax.fori_loop(0, NX, arrived, 0)
        pair_copy(k).wait_recv()
        for i in range(NX):
            q = tdot(rf[i * NZ + tz], bb[k, i, 0:2].reshape(NC * R, 2 * NE))
            real = q[:A, :NE] - q[A:, NE:]
            imag = q[:A, NE:] + q[A:, :NE]
            for j in range(NY):
                pa[k, i, j] = real[:AR, j * EQ : (j + 1) * EQ]
                if AR < A:
                    pb[k, j, i, 0 : A - AR] = real[AR:, j * EQ : (j + 1) * EQ]
                pb[k, j, i, A - AR :] = imag[:, j * EQ : (j + 1) * EQ]

        @pl.when(k == 0)
        def _():
            wa[...] = pa[0].astype(BF)

        @pl.when(k == 1)
        def _():
            wb[...] = pb[1].astype(BF)

        @pl.when(k == NZ - 1)
        def _():
            with jax.named_scope("raw_wait"):
                for copy in raw_copies():
                    copy().wait_recv()
            pa[NZ - 1] = pa[NZ - 1] + va[...].astype(F32)
            pb[NZ - 1] = pb[NZ - 1] + vb[...].astype(F32)

        firsts = first_copies(k)
        for n, (p, t, far_side) in enumerate([(pa, ta1, xo), (pb, tb1, yo)]):

            @pl.when(k != n)
            def _(n=n, p=p, t=t, far_side=far_side):
                t[k] = p[k, far_side].astype(BF)
                firsts[n]().start()
                firsts[n + 2]().start()

        @pl.when(k == RAW)
        def _():
            for copy in raw_copies():
                copy().start()

    def stage_second(k):
        firsts, seconds = first_copies(k), second_copies(k)
        for n, (p, t, r, to, half) in enumerate(
            [
                (pa, ta2, ra1, xp, 0),
                (pb, tb2, rb1, yp, 0),
                (pa, ta2, ra1, xm, 1),
                (pb, tb2, rb1, ym, 1),
            ]
        ):
            mine, rest = (slice(0, 2), slice(2, 4)) if half == 0 else (slice(2, 4), slice(0, 2))

            @pl.when(k != n % 2)
            def _(n=n, p=p, t=t, r=r, to=to, half=half, mine=mine, rest=rest):
                t[k, half, rest] = p[k, to, rest].astype(BF)
                firsts[n]().wait_recv()
                t[k, half, mine] = (p[k, to, mine] + r[k, half].astype(F32)).astype(BF)
                seconds[n]().start()

    def stage_third(k):
        seconds = second_copies(k)
        for n, (p, q, t, r, me) in enumerate([(pa, qa, tda, ra2, x), (pb, qb, tdb, rb2, y)]):

            @pl.when(k != n)
            def _(n=n, p=p, q=q, t=t, r=r, me=me):
                seconds[n]().wait_recv()
                seconds[n + 2]().wait_recv()
                q[k] = p[k, me] + r[k, 0].astype(F32) + r[k, 1].astype(F32)
                t[k] = q[k].astype(BF)
                for d in (2, 1, 3):
                    direct_copies(k, d, True)[n]().start()

    def direct_sum(k, n):
        q, r, me, size = ((qa, rda, y, NY), (qb, rdb, x, NX))[n]
        total = q[k, me]
        for d in (1, 3, 2):
            direct_copies(k, d, False)[n]().wait_recv()
            total = total + r[k, lax.rem(me + d, size)].astype(F32)
        return total

    def stage_last(k):
        for n, rows in enumerate((slice(0, AR), slice(AR, 2 * A))):

            @pl.when(k != n)
            def _(n=n, rows=rows):
                sm[k, rows] = direct_sum(k, n).astype(BF)

            @pl.when(k == n)
            def _(rows=rows):
                sm[k, rows] = jnp.zeros((rows.stop - rows.start, EQ), BF)

        z_copy(k).start()

    stages = [
        (stage_merge, LAGS[0], NZ),
        (stage_second, LAGS[2], NZ),
        (stage_third, LAGS[3], NZ),
        (stage_patterns, LAGS[1], NZ),
        (stage_last, LAGS[4], NZ - 1),
    ]

    def flow(t, carry):
        for stage, lag, count in stages:

            @pl.when(jnp.logical_and(t >= lag, t < count + lag))
            def _(stage=stage, lag=lag):
                with jax.named_scope(stage.__name__):
                    stage(t - lag)

        return carry

    lax.fori_loop(0, NZ - 1 + stages[-1][1], flow, 0)

    with jax.named_scope("d_wait"):
        total = jnp.concatenate([direct_sum(NZ - 1, n) for n in range(2)], axis=0)
    with jax.named_scope("z_wait"):
        for k in range(NZ - 1):
            z_copy(k).wait_recv()
            total = total + rz[k].astype(F32)
    intensity = total[:A] * total[:A] + total[A:] * total[A:]
    inten[...] = intensity
    save = pltpu.make_async_copy(inten, inten_hbm, ld_sem.at[6])
    save.start()
    mx[...] = jnp.max(intensity, axis=0, keepdims=True)

    near = remote(mx, m1.at[1], ms.at[0], mr.at[CHIPS], to_sib)()
    near.start()
    with jax.named_scope("near_wait"):
        near.wait_recv()
    mz[...] = jnp.maximum(mx[...], m1[1])
    m2[chip] = mz[...]

    def far(i, sender):
        other = lax.rem(chip + i, CHIPS)
        at = chip if sender else other
        return remote(mz, m2.at[at], ms.at[i], mr.at[at], (other * NC + c, y))()

    def far_wait(i, carry):
        far(i, False).wait_recv()
        return carry

    with jax.named_scope("far_send"):
        for i in range(CHIPS // 2, CHIPS // 2 + CHIPS - 1):
            far(1 + i % (CHIPS - 1), True).start()
    def drain(k, carry):
        pair_copy(k).wait_send()
        for n in range(2):

            @pl.when(k != n)
            def _(n=n):
                for copies in (first_copies(k), second_copies(k)):
                    copies[n]().wait_send()
                    copies[n + 2]().wait_send()
                for d in range(1, NX):
                    direct_copies(k, d, True)[n]().wait_send()

        @pl.when(k < NZ - 1)
        def _():
            z_copy(k).wait_send()

        return carry

    def drain_far(i, carry):
        far(i, True).wait_send()
        return carry

    with jax.named_scope("drain"):
        for i in range(CHIPS):
            if i != CHIPS - NX:
                f_copy(i).wait_send()
        lax.fori_loop(0, NZ, drain, 0)
        near.wait_send()
        for copy in raw_copies():
            copy().wait_send()

    with jax.named_scope("far_wait"):
        lax.fori_loop(1, CHIPS, far_wait, 0)
    top_out[...] = jnp.max(m2[...], axis=0)
    lax.fori_loop(1, CHIPS, drain_far, 0)
    save.wait()


def finish(inten, top, out, peak):
    peak[...] = top[...]
    out[...] = inten[...] / (top[...] + 1.0)


def body(currents, leaf_basis, leaf_box, box_count, merge_factor, angle_factor):
    turned = jnp.transpose(merge_factor, (0, 2, 1)).reshape(2 * LR, NX * GX)

    vm = pltpu.VMEM
    dma = pltpu.SemaphoreType.DMA
    anyspace = pl.BlockSpec(memory_space=pl.ANY)
    invm = pl.BlockSpec(memory_space=pltpu.VMEM)
    shapes = (
        jax.ShapeDtypeStruct((A, EQ), F32),
        jax.ShapeDtypeStruct((1, EQ), F32),
    )
    inten, top = pl.pallas_call(
        kernel,
        out_shape=shapes,
        in_specs=[anyspace] * 6,
        out_specs=(anyspace, invm),
        scratch_shapes=[
            pltpu.SMEM((LEAF,), jnp.int32),
            vm((1, S_DEV), jnp.int32),
            vm((A, EQ), F32),
            vm((S_DEV, 2 * NE), BF),
            vm((2, R, S_DEV), BF),
            vm((2 * LR, NX * GX), BF),
            vm((A, 2, NX * GX), BF),
            vm((NX * GX, 2 * A), BF),
            vm((2 * LR, S_DEV), BF),
            vm((NX * GX, 2 * LR), BF),
            vm((2 * LR, 2 * NE), BF),
            vm((NZ, NX, 3, R, 2 * NE), BF),
            vm((CHIPS, NC * R, 2 * A), BF),
            vm((NZ, NX, NY, AR, EQ), F32),
            vm((NZ, NY, NX, BR, EQ), F32),
            vm((NZ, 4, AR, EQ), BF),
            vm((NZ, 4, BR, EQ), BF),
            vm((NZ, 2, 4, AR, EQ), BF),
            vm((NZ, 2, 4, BR, EQ), BF),
            vm((NZ, 2, 2, AR, EQ), BF),
            vm((NZ, 2, 2, BR, EQ), BF),
            vm((NZ, 2, 4, AR, EQ), BF),
            vm((NZ, 2, 4, BR, EQ), BF),
            vm((NZ, NY, AR, EQ), F32),
            vm((NZ, NX, BR, EQ), F32),
            vm((NZ, 2 * A, EQ), BF),
            vm((NZ, 2 * A, EQ), BF),
            vm((NX, NY, AR, EQ), BF),
            vm((NY, NX, BR, EQ), BF),
            vm((NX, NY, AR, EQ), BF),
            vm((NY, NX, BR, EQ), BF),
            vm((NZ, NY, AR, EQ), BF),
            vm((NZ, NX, BR, EQ), BF),
            vm((NZ, NY, AR, EQ), BF),
            vm((NZ, NX, BR, EQ), BF),
            vm((1, EQ), F32),
            vm((2, 1, EQ), F32),
            vm((1, EQ), F32),
            vm((CHIPS, 1, EQ), F32),
            dma((7,)),
            dma((CHIPS,)),
            dma((CHIPS,)),
            dma((NZ,)),
            dma((NZ,)),
            dma((NZ, 8)),
            dma((NZ, 8)),
            dma((NZ,)),
            dma((NZ,)),
            dma((NZ, NX + NY)),
            dma((NZ, NX + NY)),
            dma((2,)),
            dma((2,)),
            dma((CHIPS,)),
            dma((CHIPS + 1,)),
        ],
        compiler_params=pltpu.CompilerParams(
            collective_id=0, has_side_effects=True, vmem_limit_bytes=62 * 1024 * 1024
        ),
    )(
        box_count,
        leaf_box.reshape(1, S_DEV),
        currents,
        leaf_basis,
        turned,
        angle_factor,
    )
    normalized, peak = pl.pallas_call(
        finish,
        out_shape=shapes,
        in_specs=[invm, invm],
        out_specs=(invm, invm),
    )(inten, top)
    return normalized, peak.reshape(EQ)


def solution(mesh):
    in_specs = (
        P(("src", "grp"), None),
        P(None, None, ("src", "grp")),
        P(("src", "grp")),
        P(("src", "grp")),
        P(None, None, ("src", "grp")),
        P("src", None, None, None),
    )
    out_specs = (P("src", "grp"), P("grp"))
    return jax.shard_map(body, mesh=mesh, in_specs=in_specs, out_specs=out_specs, check_vma=False)
```

```python
import functools

import jax
import jax.numpy as jnp
from jax import lax
from jax.experimental import pallas as pl
from jax.experimental.pallas import tpu as pltpu
from jax.sharding import PartitionSpec as P

MESH = pl.DeviceIdType.MESH
BF = jnp.bfloat16
F32 = jnp.float32

NX, NY, NZ, NC = 4, 4, 8, 2
CHIPS = NX * NZ
R = 40
LEAF = 8
S_DEV = 2048
NE = 512
A = 64
EQ = NE // NY
LR = LEAF * R
GX = NZ * NC * R
OFFSETS = (1, 7, 2, 5, 3, 4, 6, 0)
LAGS = (0, 1, 4, 7, 10)
AR = 64
BR = 2 * A - AR
RAW = 4


def tdot(a, b):
    return lax.dot_general(a, b, (((0,), (0,)), ((), ())), preferred_element_type=F32)


def dot(a, b):
    return jnp.dot(a, b, preferred_element_type=F32)


def kernel(
    cnt_hbm,
    box_hbm,
    x_hbm,
    basis_hbm,
    mt_hbm,
    own_hbm,
    inten_hbm,
    top_out,
    cnt,
    box,
    inten,
    xv,
    basis,
    mt,
    own,
    ft,
    lmat,
    mm,
    rhs,
    bb,
    rf,
    pa,
    pb,
    ta1,
    tb1,
    ta2,
    tb2,
    ra1,
    rb1,
    ra2,
    rb2,
    qa,
    qb,
    sm,
    rz,
    wa,
    wb,
    va,
    vb,
    tda,
    tdb,
    rda,
    rdb,
    mx,
    m1,
    mz,
    m2,
    ld_sem,
    fs_sem,
    fr_sem,
    ps_sem,
    pr_sem,
    s1,
    r1,
    zs,
    zr,
    ds,
    dr,
    ws,
    wr,
    ms,
    mr,
):
    src = lax.axis_index("src")
    y = lax.axis_index("grp")
    c = lax.rem(src, NC)
    z = lax.rem(src // NC, NZ)
    x = src // (NC * NZ)
    chip = src // NC
    mm4 = mm.reshape(NX, NZ, NC * R, 2 * LR)
    ft3 = ft.reshape(CHIPS, NC * R, 2 * A)

    def dev(xx, yy, zz, cc):
        return ((xx * NZ + zz) * NC + cc, yy)

    def remote(a, b, send, recv, to):
        return lambda: pltpu.make_async_remote_copy(
            src_ref=a,
            dst_ref=b,
            send_sem=send,
            recv_sem=recv,
            device_id=to,
            device_id_type=MESH,
        )

    def target_z(k):
        if isinstance(k, int):
            return lax.rem(z + OFFSETS[k], NZ)
        packed = jnp.int32(sum(o * NZ**i for i, o in enumerate(OFFSETS)))
        return lax.rem(z + lax.rem(lax.shift_right_logical(packed, 3 * k), NZ), NZ)

    xp, xm, xo = lax.rem(x + 1, NX), lax.rem(x + 3, NX), lax.rem(x + 2, NX)
    yp, ym, yo = lax.rem(y + 1, NY), lax.rem(y + 3, NY), lax.rem(y + 2, NY)
    to_xp, to_xm = dev(xp, y, z, c), dev(xm, y, z, c)
    to_yp, to_ym = dev(x, yp, z, c), dev(x, ym, z, c)
    to_sib = dev(x, y, z, 1 - c)

    loads = [
        pltpu.make_async_copy(a, b, ld_sem.at[i])
        for i, (a, b) in enumerate(
            [
                (own_hbm.at[:, y], own),
                (cnt_hbm, cnt),
                (box_hbm, box),
                (basis_hbm, basis),
                (x_hbm, xv),
                (mt_hbm, mt),
            ]
        )
    ]
    for copy in loads:
        copy.start()

    barrier = pltpu.get_barrier_semaphore()

    def greet(i, carry):
        other = lax.rem(chip + i, CHIPS)
        pl.semaphore_signal(
            barrier, inc=1, device_id=(other * NC + c, y), device_id_type=MESH
        )
        return carry

    lax.fori_loop(1, CHIPS, greet, 0)
    greeted = [to_yp, to_ym, dev(x, yo, z, c), to_sib]
    for to in greeted:
        pl.semaphore_signal(barrier, inc=1, device_id=to, device_id_type=MESH)

    with jax.named_scope("turn_f"):
        loads[0].wait()

        for i in range(NX * GX // 128):
            span = slice(i * 128, (i + 1) * 128)
            pair = own[:, :, span]
            both = jnp.concatenate([pair[:, 0, :], pair[:, 1, :]], axis=0)
            ft[span, :] = jnp.transpose(both)
        rf[chip] = ft3[chip]

    with jax.named_scope("build"):
        for copy in loads[1:4]:
            copy.wait()
        scale = [
            lax.rsqrt(jnp.full((8, 128), cnt[b], jnp.int32).astype(F32))[0:1, 0:1]
            for b in range(LEAF)
        ]
        width = 256

        def build(i, carry):
            cols = pl.ds(pl.multiple_of(i * width, width), width)
            where = box[:, cols]
            gains = [
                jnp.where(where == b, jnp.broadcast_to(scale[b], (1, width)), 0.0)
                for b in range(LEAF)
            ]
            for p in range(2):
                wide = basis[p, :, cols].astype(F32)
                rows = jnp.concatenate([wide * g for g in gains], axis=0)
                lmat[p * LR : (p + 1) * LR, cols] = rows.astype(BF)
            return carry

        lax.fori_loop(0, S_DEV // width, build, 0)

    with jax.named_scope("barrier"):
        pl.semaphore_wait(barrier, CHIPS - 1 + len(greeted))

    def f_copy(i):
        k, dx = i // NX, i % NX
        tx, tz = lax.rem(x + dx, NX), lax.rem(z + NZ - OFFSETS[k], NZ)
        return remote(
            ft3.at[tx * NZ + tz], rf.at[chip], fs_sem.at[0], fr_sem.at[z], dev(tx, y, tz, c)
        )()

    with jax.named_scope("f_send"):
        for i in range(CHIPS):
            if i != CHIPS - NX:
                f_copy(i).start()

    tile = 256
    with jax.named_scope("leaf"):
        loads[4].wait()
        loads[5].wait()
        turns = NX * GX // 128 // (NE // tile)

        def leaf(i, carry):
            for n in range(turns):
                span = pl.ds(pl.multiple_of((i * turns + n) * 128, 128), 128)
                mm[span, :] = jnp.transpose(mt[:, span])
            lo = pl.ds(pl.multiple_of(i * tile, tile), tile)
            hi = pl.ds(pl.multiple_of(NE + i * tile, tile), tile)
            u = dot(lmat[...], xv[:, lo])
            w = dot(lmat[...], xv[:, hi])
            real = (u[:LR] - w[LR:]).astype(BF)
            imag = (w[:LR] + u[LR:]).astype(BF)
            rhs[:LR, lo] = real
            rhs[LR:, hi] = real
            rhs[:LR, hi] = imag
            rhs[LR:, lo] = -imag
            return carry

        lax.fori_loop(0, NE // tile, leaf, 0)

    def bulk(ref, send, recv):
        return remote(ref, ref, send, recv, to_sib)()

    def pair_copy(k):
        return remote(bb.at[k, :, 2], bb.at[k, :, c], ps_sem.at[0], pr_sem.at[k], to_sib)()

    def first_copies(k):
        return [
            remote(ta1.at[k, 0:2], ra1.at[k, 0], s1.at[0], r1.at[k, 0], to_xp),
            remote(tb1.at[k, 0:2], rb1.at[k, 0], s1.at[1], r1.at[k, 1], to_yp),
            remote(ta1.at[k, 2:4], ra1.at[k, 1], s1.at[0], r1.at[k, 2], to_xm),
            remote(tb1.at[k, 2:4], rb1.at[k, 1], s1.at[1], r1.at[k, 3], to_ym),
        ]

    def second_copies(k):
        return [
            remote(ta2.at[k, 0], ra2.at[k, 0], s1.at[2], r1.at[k, 4], to_xp),
            remote(tb2.at[k, 0], rb2.at[k, 0], s1.at[3], r1.at[k, 5], to_yp),
            remote(ta2.at[k, 1], ra2.at[k, 1], s1.at[2], r1.at[k, 4], to_xm),
            remote(tb2.at[k, 1], rb2.at[k, 1], s1.at[3], r1.at[k, 5], to_ym),
        ]

    def direct_copies(k, d, sender):
        oy, ox = lax.rem(y + d, NY), lax.rem(x + d, NX)
        ty, tx = (y, x) if sender else (oy, ox)
        return [
            remote(
                tda.at[k, oy],
                rda.at[k, ty],
                ds.at[0],
                dr.at[k, 0],
                dev(x, oy, z, c),
            ),
            remote(
                tdb.at[k, ox],
                rdb.at[k, tx],
                ds.at[1],
                dr.at[k, 1],
                dev(ox, y, z, c),
            ),
        ]

    def raw_copies():
        up, down = lax.rem(z + 1, NZ), lax.rem(z + NZ - 1, NZ)
        return [
            remote(wa, va, ws.at[0], wr.at[0], dev(x, y, up, c)),
            remote(wb, vb, ws.at[1], wr.at[1], dev(x, y, down, c)),
        ]

    def z_copy(k):
        return remote(sm.at[k], rz.at[k], zs.at[0], zr.at[0], dev(x, y, target_z(k), c))()

    def stage_merge(k):
        left = mm4[:, target_z(k)].reshape(NX * NC * R, 2 * LR)
        for n in range(2 * NE // tile):
            cols = slice(n * tile, (n + 1) * tile)
            v = dot(left, rhs[:, cols])
            for i in range(NX):
                bb[k, i, 2 * c, :, cols] = v[2 * i * R : (2 * i + 1) * R].astype(BF)
                bb[k, i, 2 - c, :, cols] = v[(2 * i + 1) * R : (2 * i + 2) * R].astype(BF)
        pair_copy(k).start()

    def stage_patterns(k):
        tz = target_z(k)

        @pl.when(k < NZ - 1)
        def _():
            bulk(rf.at[pl.ds(0, NX)], fs_sem.at[0], fr_sem.at[tz]).wait_recv()

        @pl.when(k == NZ - 1)
        def _():
            bulk(rf.at[pl.ds(0, NX - 1)], fs_sem.at[0], fr_sem.at[tz]).wait_recv()

        pair_copy(k).wait_recv()
        for i in range(NX):
            q = tdot(rf[i * NZ + tz], bb[k, i, 0:2].reshape(NC * R, 2 * NE))
            real = q[:A, :NE] - q[A:, NE:]
            imag = q[:A, NE:] + q[A:, :NE]
            for j in range(NY):
                pa[k, i, j] = real[:AR, j * EQ : (j + 1) * EQ]
                if AR < A:
                    pb[k, j, i, 0 : A - AR] = real[AR:, j * EQ : (j + 1) * EQ]
                pb[k, j, i, A - AR :] = imag[:, j * EQ : (j + 1) * EQ]

        @pl.when(k == 0)
        def _():
            wa[...] = pa[0].astype(BF)

        @pl.when(k == 1)
        def _():
            wb[...] = pb[1].astype(BF)

        @pl.when(k == NZ - 1)
        def _():
            with jax.named_scope("raw_wait"):
                for copy in raw_copies():
                    copy().wait_recv()
            pa[NZ - 1] = pa[NZ - 1] + va[...].astype(F32)
            pb[NZ - 1] = pb[NZ - 1] + vb[...].astype(F32)

        firsts = first_copies(k)
        for n, (p, t, far_side) in enumerate([(pa, ta1, xo), (pb, tb1, yo)]):

            @pl.when(k != n)
            def _(n=n, p=p, t=t, far_side=far_side):
                t[k] = p[k, far_side].astype(BF)
                firsts[n]().start()
                firsts[n + 2]().start()

        @pl.when(k == RAW)
        def _():
            for copy in raw_copies():
                copy().start()

    def stage_second(k):
        firsts, seconds = first_copies(k), second_copies(k)
        for n, (p, t, r, to, half) in enumerate(
            [
                (pa, ta2, ra1, xp, 0),
                (pb, tb2, rb1, yp, 0),
                (pa, ta2, ra1, xm, 1),
                (pb, tb2, rb1, ym, 1),
            ]
        ):
            mine, rest = (slice(0, 2), slice(2, 4)) if half == 0 else (slice(2, 4), slice(0, 2))

            @pl.when(k != n % 2)
            def _(n=n, p=p, t=t, r=r, to=to, half=half, mine=mine, rest=rest):
                t[k, half, rest] = p[k, to, rest].astype(BF)
                firsts[n]().wait_recv()
                t[k, half, mine] = (p[k, to, mine] + r[k, half].astype(F32)).astype(BF)
                seconds[n]().start()

    def stage_third(k):
        for n, (p, q, t, r, me) in enumerate([(pa, qa, tda, ra2, x), (pb, qb, tdb, rb2, y)]):

            @pl.when(k != n)
            def _(n=n, p=p, q=q, t=t, r=r, me=me):
                bulk(r.at[k], s1.at[2 + n], r1.at[k, 4 + n]).wait_recv()
                q[k] = p[k, me] + r[k, 0].astype(F32) + r[k, 1].astype(F32)
                t[k] = q[k].astype(BF)
                for d in (2, 1, 3):
                    direct_copies(k, d, True)[n]().start()

    def direct_sum(k, n):
        q, r, me, size = ((qa, rda, y, NY), (qb, rdb, x, NX))[n]
        total = q[k, me]
        bulk(r.at[k, pl.ds(0, NX - 1)], ds.at[n], dr.at[k, n]).wait_recv()
        for d in (1, 3, 2):
            total = total + r[k, lax.rem(me + d, size)].astype(F32)
        return total

    def stage_last(k):
        for n, rows in enumerate((slice(0, AR), slice(AR, 2 * A))):

            @pl.when(k != n)
            def _(n=n, rows=rows):
                sm[k, rows] = direct_sum(k, n).astype(BF)

            @pl.when(k == n)
            def _(rows=rows):
                sm[k, rows] = jnp.zeros((rows.stop - rows.start, EQ), BF)

        z_copy(k).start()

    stages = [
        (stage_merge, LAGS[0], NZ),
        (stage_second, LAGS[2], NZ),
        (stage_third, LAGS[3], NZ),
        (stage_patterns, LAGS[1], NZ),
        (stage_last, LAGS[4], NZ - 1),
    ]

    def flow(t, carry):
        for stage, lag, count in stages:

            @pl.when(jnp.logical_and(t >= lag, t < count + lag))
            def _(stage=stage, lag=lag):
                with jax.named_scope(stage.__name__):
                    stage(t - lag)

        return carry

    lax.fori_loop(0, NZ - 1 + stages[-1][1], flow, 0)

    with jax.named_scope("d_wait"):
        total = jnp.concatenate([direct_sum(NZ - 1, n) for n in range(2)], axis=0)
    with jax.named_scope("z_wait"):
        bulk(rz.at[pl.ds(0, NZ - 1)], zs.at[0], zr.at[0]).wait_recv()
        for k in range(NZ - 1):
            total = total + rz[k].astype(F32)
    intensity = total[:A] * total[:A] + total[A:] * total[A:]
    inten[...] = intensity
    save = pltpu.make_async_copy(inten, inten_hbm, ld_sem.at[6])
    save.start()
    mx[...] = jnp.max(intensity, axis=0, keepdims=True)

    near = remote(mx, m1.at[1], ms.at[0], mr.at[0], to_sib)()
    near.start()
    with jax.named_scope("near_wait"):
        near.wait_recv()
    mz[...] = jnp.maximum(mx[...], m1[1])
    m2[chip] = mz[...]

    def far(i):
        other = lax.rem(chip + i, CHIPS)
        return remote(mz, m2.at[chip], ms.at[1], mr.at[1], (other * NC + c, y))()

    everyone = bulk(m2.at[pl.ds(0, CHIPS - 1)], ms.at[1], mr.at[1])
    with jax.named_scope("far_send"):
        for i in range(CHIPS // 2, CHIPS // 2 + CHIPS - 1):
            far(1 + i % (CHIPS - 1)).start()
    with jax.named_scope("drain"):
        bulk(ft3.at[pl.ds(0, CHIPS - 1)], fs_sem.at[0], fr_sem.at[0]).wait_send()
        bulk(bb.at[:, :, 2], ps_sem.at[0], pr_sem.at[0]).wait_send()
        sent = pl.ds(1, NZ - 1)
        for n, (t1, t2, td) in enumerate([(ta1, ta2, tda), (tb1, tb2, tdb)]):
            bulk(t1.at[sent], s1.at[n], r1.at[0, 0]).wait_send()
            bulk(t2.at[sent], s1.at[2 + n], r1.at[0, 0]).wait_send()
            bulk(td.at[sent, pl.ds(0, NX - 1)], ds.at[n], dr.at[0, 0]).wait_send()
        bulk(sm.at[pl.ds(0, NZ - 1)], zs.at[0], zr.at[0]).wait_send()
        near.wait_send()
        for copy in raw_copies():
            copy().wait_send()

    with jax.named_scope("far_wait"):
        everyone.wait_recv()
    top_out[...] = jnp.max(m2[...], axis=0)
    everyone.wait_send()
    save.wait()


def finish(inten, top, out, peak):
    peak[...] = top[...]
    out[...] = inten[...] / (top[...] + 1.0)


def body(currents, leaf_basis, leaf_box, box_count, merge_factor, angle_factor):
    turned = jnp.transpose(merge_factor, (0, 2, 1)).reshape(2 * LR, NX * GX)

    vm = pltpu.VMEM
    dma = pltpu.SemaphoreType.DMA
    anyspace = pl.BlockSpec(memory_space=pl.ANY)
    invm = pl.BlockSpec(memory_space=pltpu.VMEM)
    shapes = (
        jax.ShapeDtypeStruct((A, EQ), F32),
        jax.ShapeDtypeStruct((1, EQ), F32),
    )
    inten, top = pl.pallas_call(
        kernel,
        out_shape=shapes,
        in_specs=[anyspace] * 6,
        out_specs=(anyspace, invm),
        scratch_shapes=[
            pltpu.SMEM((LEAF,), jnp.int32),
            vm((1, S_DEV), jnp.int32),
            vm((A, EQ), F32),
            vm((S_DEV, 2 * NE), BF),
            vm((2, R, S_DEV), BF),
            vm((2 * LR, NX * GX), BF),
            vm((A, 2, NX * GX), BF),
            vm((NX * GX, 2 * A), BF),
            vm((2 * LR, S_DEV), BF),
            vm((NX * GX, 2 * LR), BF),
            vm((2 * LR, 2 * NE), BF),
            vm((NZ, NX, 3, R, 2 * NE), BF),
            vm((CHIPS, NC * R, 2 * A), BF),
            vm((NZ, NX, NY, AR, EQ), F32),
            vm((NZ, NY, NX, BR, EQ), F32),
            vm((NZ, 4, AR, EQ), BF),
            vm((NZ, 4, BR, EQ), BF),
            vm((NZ, 2, 4, AR, EQ), BF),
            vm((NZ, 2, 4, BR, EQ), BF),
            vm((NZ, 2, 2, AR, EQ), BF),
            vm((NZ, 2, 2, BR, EQ), BF),
            vm((NZ, 2, 4, AR, EQ), BF),
            vm((NZ, 2, 4, BR, EQ), BF),
            vm((NZ, NY, AR, EQ), F32),
            vm((NZ, NX, BR, EQ), F32),
            vm((NZ, 2 * A, EQ), BF),
            vm((NZ, 2 * A, EQ), BF),
            vm((NX, NY, AR, EQ), BF),
            vm((NY, NX, BR, EQ), BF),
            vm((NX, NY, AR, EQ), BF),
            vm((NY, NX, BR, EQ), BF),
            vm((NZ, NY, AR, EQ), BF),
            vm((NZ, NX, BR, EQ), BF),
            vm((NZ, NY, AR, EQ), BF),
            vm((NZ, NX, BR, EQ), BF),
            vm((1, EQ), F32),
            vm((2, 1, EQ), F32),
            vm((1, EQ), F32),
            vm((CHIPS, 1, EQ), F32),
            dma((7,)),
            dma((1,)),
            dma((NZ,)),
            dma((1,)),
            dma((NZ,)),
            dma((4,)),
            dma((NZ, 6)),
            dma((1,)),
            dma((1,)),
            dma((2,)),
            dma((NZ, 2)),
            dma((2,)),
            dma((2,)),
            dma((2,)),
            dma((2,)),
        ],
        compiler_params=pltpu.CompilerParams(
            collective_id=0, has_side_effects=True, vmem_limit_bytes=62 * 1024 * 1024
        ),
    )(
        box_count,
        leaf_box.reshape(1, S_DEV),
        currents,
        leaf_basis,
        turned,
        angle_factor,
    )
    normalized, peak = pl.pallas_call(
        finish,
        out_shape=shapes,
        in_specs=[invm, invm],
        out_specs=(invm, invm),
    )(inten, top)
    return normalized, peak.reshape(EQ)


def solution(mesh):
    in_specs = (
        P(("src", "grp"), None),
        P(None, None, ("src", "grp")),
        P(("src", "grp")),
        P(("src", "grp")),
        P(None, None, ("src", "grp")),
        P("src", None, None, None),
    )
    out_specs = (P("src", "grp"), P("grp"))
    return jax.shard_map(body, mesh=mesh, in_specs=in_specs, out_specs=out_specs, check_vma=False)
```

```python
import functools

import jax
import jax.numpy as jnp
from jax import lax
from jax.experimental import pallas as pl
from jax.experimental.pallas import tpu as pltpu
from jax.sharding import PartitionSpec as P

MESH = pl.DeviceIdType.MESH
BF = jnp.bfloat16
F32 = jnp.float32

NX, NY, NZ, NC = 4, 4, 8, 2
CHIPS = NX * NZ
R = 40
LEAF = 8
S_DEV = 2048
NE = 512
A = 64
EQ = NE // NY
LR = LEAF * R
GX = NZ * NC * R
OFFSETS = (1, 7, 2, 5, 3, 4, 6, 0)
LAGS = (0, 1, 4, 7, 10)
AR = 64
BR = 2 * A - AR
RAW = 4


def tdot(a, b):
    return lax.dot_general(a, b, (((0,), (0,)), ((), ())), preferred_element_type=F32)


def dot(a, b):
    return jnp.dot(a, b, preferred_element_type=F32)


def kernel(
    cnt_hbm,
    box_hbm,
    x_hbm,
    basis_hbm,
    mt_hbm,
    own_hbm,
    inten_hbm,
    top_out,
    cnt,
    box,
    inten,
    xv,
    basis,
    mt,
    own,
    ft,
    lmat,
    mm,
    rhs,
    bb,
    rf,
    pa,
    pb,
    ta1,
    tb1,
    ta2,
    tb2,
    ra1,
    rb1,
    ra2,
    rb2,
    qa,
    qb,
    sm,
    rz,
    wa,
    wb,
    va,
    vb,
    tda,
    tdb,
    rda,
    rdb,
    mx,
    m1,
    mz,
    m2,
    ld_sem,
    fs_sem,
    fr_sem,
    ps_sem,
    pr_sem,
    s1,
    r1,
    zs,
    zr,
    ds,
    dr,
    ws,
    wr,
    ms,
    mr,
):
    src = lax.axis_index("src")
    y = lax.axis_index("grp")
    c = lax.rem(src, NC)
    z = lax.rem(src // NC, NZ)
    x = src // (NC * NZ)
    chip = src // NC
    mm4 = mm.reshape(NX, NZ, NC * R, 2 * LR)
    ft3 = ft.reshape(CHIPS, NC * R, 2 * A)

    def dev(xx, yy, zz, cc):
        return ((xx * NZ + zz) * NC + cc, yy)

    def remote(a, b, send, recv, to):
        return lambda: pltpu.make_async_remote_copy(
            src_ref=a,
            dst_ref=b,
            send_sem=send,
            recv_sem=recv,
            device_id=to,
            device_id_type=MESH,
        )

    def target_z(k):
        if isinstance(k, int):
            return lax.rem(z + OFFSETS[k], NZ)
        packed = jnp.int32(sum(o * NZ**i for i, o in enumerate(OFFSETS)))
        return lax.rem(z + lax.rem(lax.shift_right_logical(packed, 3 * k), NZ), NZ)

    xp, xm, xo = lax.rem(x + 1, NX), lax.rem(x + 3, NX), lax.rem(x + 2, NX)
    yp, ym, yo = lax.rem(y + 1, NY), lax.rem(y + 3, NY), lax.rem(y + 2, NY)
    to_xp, to_xm = dev(xp, y, z, c), dev(xm, y, z, c)
    to_yp, to_ym = dev(x, yp, z, c), dev(x, ym, z, c)
    to_sib = dev(x, y, z, 1 - c)

    loads = [
        pltpu.make_async_copy(a, b, ld_sem.at[i])
        for i, (a, b) in enumerate(
            [
                (own_hbm.at[:, y], own),
                (cnt_hbm, cnt),
                (box_hbm, box),
                (basis_hbm, basis),
                (x_hbm, xv),
                (mt_hbm, mt),
            ]
        )
    ]
    for copy in loads:
        copy.start()

    barrier = pltpu.get_barrier_semaphore()

    for i in range(1, CHIPS):
        pl.semaphore_signal(
            barrier,
            inc=1,
            device_id=(lax.rem(chip + i, CHIPS) * NC + c, y),
            device_id_type=MESH,
        )
    greeted = [to_yp, to_ym, dev(x, yo, z, c), to_sib]
    for to in greeted:
        pl.semaphore_signal(barrier, inc=1, device_id=to, device_id_type=MESH)

    with jax.named_scope("turn_f"):
        loads[0].wait()

        for i in range(NX * GX // 128):
            span = slice(i * 128, (i + 1) * 128)
            pair = own[:, :, span]
            both = jnp.concatenate([pair[:, 0, :], pair[:, 1, :]], axis=0)
            ft[span, :] = jnp.transpose(both)
        rf[chip] = ft3[chip]

    with jax.named_scope("build"):
        for copy in loads[1:4]:
            copy.wait()
        scale = [
            lax.rsqrt(jnp.full((8, 128), cnt[b], jnp.int32).astype(F32))[0:1, 0:1]
            for b in range(LEAF)
        ]
        width = 256

        def build(i, carry):
            cols = pl.ds(pl.multiple_of(i * width, width), width)
            where = box[:, cols]
            gains = [
                jnp.where(where == b, jnp.broadcast_to(scale[b], (1, width)), 0.0)
                for b in range(LEAF)
            ]
            for p in range(2):
                wide = basis[p, :, cols].astype(F32)
                rows = jnp.concatenate([wide * g for g in gains], axis=0)
                lmat[p * LR : (p + 1) * LR, cols] = rows.astype(BF)
            return carry

        lax.fori_loop(0, S_DEV // width, build, 0)

    with jax.named_scope("barrier"):
        pl.semaphore_wait(barrier, CHIPS - 1 + len(greeted))

    def f_copy(i):
        k, dx = i // NX, i % NX
        tx, tz = lax.rem(x + dx, NX), lax.rem(z + NZ - OFFSETS[k], NZ)
        return remote(
            ft3.at[tx * NZ + tz], rf.at[chip], fs_sem.at[0], fr_sem.at[z], dev(tx, y, tz, c)
        )()

    with jax.named_scope("f_send"):
        for i in range(CHIPS):
            if i != CHIPS - NX:
                f_copy(i).start()

    tile = 256
    with jax.named_scope("leaf"):
        loads[4].wait()
        loads[5].wait()
        turns = NX * GX // 128 // (NE // tile)

        def leaf(i, carry):
            for n in range(turns):
                span = pl.ds(pl.multiple_of((i * turns + n) * 128, 128), 128)
                mm[span, :] = jnp.transpose(mt[:, span])
            lo = pl.ds(pl.multiple_of(i * tile, tile), tile)
            hi = pl.ds(pl.multiple_of(NE + i * tile, tile), tile)
            u = dot(lmat[...], xv[:, lo])
            w = dot(lmat[...], xv[:, hi])
            real = (u[:LR] - w[LR:]).astype(BF)
            imag = (w[:LR] + u[LR:]).astype(BF)
            rhs[:LR, lo] = real
            rhs[LR:, hi] = real
            rhs[:LR, hi] = imag
            rhs[LR:, lo] = -imag
            return carry

        lax.fori_loop(0, NE // tile, leaf, 0)

    def bulk(ref, send, recv):
        return remote(ref, ref, send, recv, to_sib)()

    def pair_copy(k):
        return remote(bb.at[k, :, 2], bb.at[k, :, c], ps_sem.at[0], pr_sem.at[k], to_sib)()

    def first_copies(k):
        return [
            remote(ta1.at[k, 0:2], ra1.at[k, 0], s1.at[0], r1.at[k, 0], to_xp),
            remote(tb1.at[k, 0:2], rb1.at[k, 0], s1.at[1], r1.at[k, 1], to_yp),
            remote(ta1.at[k, 2:4], ra1.at[k, 1], s1.at[0], r1.at[k, 0], to_xm),
            remote(tb1.at[k, 2:4], rb1.at[k, 1], s1.at[1], r1.at[k, 1], to_ym),
        ]

    def second_copies(k):
        return [
            remote(ta2.at[k, 0], ra2.at[k, 0], s1.at[2], r1.at[k, 2], to_xp),
            remote(tb2.at[k, 0], rb2.at[k, 0], s1.at[3], r1.at[k, 3], to_yp),
            remote(ta2.at[k, 1], ra2.at[k, 1], s1.at[2], r1.at[k, 2], to_xm),
            remote(tb2.at[k, 1], rb2.at[k, 1], s1.at[3], r1.at[k, 3], to_ym),
        ]

    def direct_copies(k, d, sender):
        oy, ox = lax.rem(y + d, NY), lax.rem(x + d, NX)
        ty, tx = (y, x) if sender else (oy, ox)
        return [
            remote(
                tda.at[k, oy],
                rda.at[k, ty],
                ds.at[0],
                dr.at[k, 0],
                dev(x, oy, z, c),
            ),
            remote(
                tdb.at[k, ox],
                rdb.at[k, tx],
                ds.at[1],
                dr.at[k, 1],
                dev(ox, y, z, c),
            ),
        ]

    def raw_copies():
        up, down = lax.rem(z + 1, NZ), lax.rem(z + NZ - 1, NZ)
        return [
            remote(wa, va, ws.at[0], wr.at[0], dev(x, y, up, c)),
            remote(wb, vb, ws.at[1], wr.at[1], dev(x, y, down, c)),
        ]

    def z_copy(k):
        return remote(sm.at[k], rz.at[k], zs.at[0], zr.at[0], dev(x, y, target_z(k), c))()

    def stage_merge(k):
        left = mm4[:, target_z(k)].reshape(NX * NC * R, 2 * LR)
        for n in range(2 * NE // tile):
            cols = slice(n * tile, (n + 1) * tile)
            v = dot(left, rhs[:, cols])
            for i in range(NX):
                bb[k, i, 2 * c, :, cols] = v[2 * i * R : (2 * i + 1) * R].astype(BF)
                bb[k, i, 2 - c, :, cols] = v[(2 * i + 1) * R : (2 * i + 2) * R].astype(BF)
        pair_copy(k).start()

    def stage_patterns(k):
        tz = target_z(k)

        @pl.when(k < NZ - 1)
        def _():
            bulk(rf.at[pl.ds(0, NX)], fs_sem.at[0], fr_sem.at[tz]).wait_recv()

        @pl.when(k == NZ - 1)
        def _():
            bulk(rf.at[pl.ds(0, NX - 1)], fs_sem.at[0], fr_sem.at[tz]).wait_recv()

        pair_copy(k).wait_recv()
        for i in range(NX):
            q = tdot(rf[i * NZ + tz], bb[k, i, 0:2].reshape(NC * R, 2 * NE))
            real = q[:A, :NE] - q[A:, NE:]
            imag = q[:A, NE:] + q[A:, :NE]
            for j in range(NY):
                pa[k, i, j] = real[:AR, j * EQ : (j + 1) * EQ]
                if AR < A:
                    pb[k, j, i, 0 : A - AR] = real[AR:, j * EQ : (j + 1) * EQ]
                pb[k, j, i, A - AR :] = imag[:, j * EQ : (j + 1) * EQ]

        @pl.when(k == 0)
        def _():
            wa[...] = pa[0].astype(BF)

        @pl.when(k == 1)
        def _():
            wb[...] = pb[1].astype(BF)

        @pl.when(k == NZ - 1)
        def _():
            with jax.named_scope("raw_wait"):
                for copy in raw_copies():
                    copy().wait_recv()
            pa[NZ - 1] = pa[NZ - 1] + va[...].astype(F32)
            pb[NZ - 1] = pb[NZ - 1] + vb[...].astype(F32)

        firsts = first_copies(k)
        for n, (p, t, far_side) in enumerate([(pa, ta1, xo), (pb, tb1, yo)]):

            @pl.when(k != n)
            def _(n=n, p=p, t=t, far_side=far_side):
                t[k] = p[k, far_side].astype(BF)
                firsts[n]().start()
                firsts[n + 2]().start()

        @pl.when(k == RAW)
        def _():
            for copy in raw_copies():
                copy().start()

    def stage_second(k):
        seconds = second_copies(k)
        for n, (p, t, r, to, half) in enumerate(
            [
                (pa, ta2, ra1, xp, 0),
                (pb, tb2, rb1, yp, 0),
                (pa, ta2, ra1, xm, 1),
                (pb, tb2, rb1, ym, 1),
            ]
        ):
            mine, rest = (slice(0, 2), slice(2, 4)) if half == 0 else (slice(2, 4), slice(0, 2))

            @pl.when(k != n % 2)
            def _(n=n, p=p, t=t, r=r, to=to, half=half, mine=mine, rest=rest):
                t[k, half, rest] = p[k, to, rest].astype(BF)
                if half == 0:
                    bulk(r.at[k], s1.at[n], r1.at[k, n]).wait_recv()
                t[k, half, mine] = (p[k, to, mine] + r[k, half].astype(F32)).astype(BF)
                seconds[n]().start()

    def stage_third(k):
        for n, (p, q, t, r, me) in enumerate([(pa, qa, tda, ra2, x), (pb, qb, tdb, rb2, y)]):

            @pl.when(k != n)
            def _(n=n, p=p, q=q, t=t, r=r, me=me):
                bulk(r.at[k], s1.at[2 + n], r1.at[k, 2 + n]).wait_recv()
                q[k] = p[k, me] + r[k, 0].astype(F32) + r[k, 1].astype(F32)
                t[k] = q[k].astype(BF)
                for d in (2, 1, 3):
                    direct_copies(k, d, True)[n]().start()

    def direct_sum(k, n):
        q, r, me, size = ((qa, rda, y, NY), (qb, rdb, x, NX))[n]
        total = q[k, me]
        bulk(r.at[k, pl.ds(0, NX - 1)], ds.at[n], dr.at[k, n]).wait_recv()
        for d in (1, 3, 2):
            total = total + r[k, lax.rem(me + d, size)].astype(F32)
        return total

    def stage_last(k):
        for n, rows in enumerate((slice(0, AR), slice(AR, 2 * A))):

            @pl.when(k != n)
            def _(n=n, rows=rows):
                sm[k, rows] = direct_sum(k, n).astype(BF)

            @pl.when(k == n)
            def _(rows=rows):
                sm[k, rows] = jnp.zeros((rows.stop - rows.start, EQ), BF)

        z_copy(k).start()

    stages = [
        (stage_merge, LAGS[0], NZ),
        (stage_second, LAGS[2], NZ),
        (stage_third, LAGS[3], NZ),
        (stage_patterns, LAGS[1], NZ),
        (stage_last, LAGS[4], NZ - 1),
    ]

    def flow(t, carry):
        for stage, lag, count in stages:

            @pl.when(jnp.logical_and(t >= lag, t < count + lag))
            def _(stage=stage, lag=lag):
                with jax.named_scope(stage.__name__):
                    stage(t - lag)

        return carry

    lax.fori_loop(0, NZ - 1 + stages[-1][1], flow, 0)

    with jax.named_scope("d_wait"):
        total = jnp.concatenate([direct_sum(NZ - 1, n) for n in range(2)], axis=0)
    with jax.named_scope("z_wait"):
        bulk(rz.at[pl.ds(0, NZ - 1)], zs.at[0], zr.at[0]).wait_recv()
        for k in range(NZ - 1):
            total = total + rz[k].astype(F32)
    intensity = total[:A] * total[:A] + total[A:] * total[A:]
    inten[...] = intensity
    save = pltpu.make_async_copy(inten, inten_hbm, ld_sem.at[6])
    save.start()
    mx[...] = jnp.max(intensity, axis=0, keepdims=True)

    near = remote(mx, m1.at[1], ms.at[0], mr.at[0], to_sib)()
    near.start()
    with jax.named_scope("near_wait"):
        near.wait_recv()
    mz[...] = jnp.maximum(mx[...], m1[1])
    m2[chip] = mz[...]

    def far(i):
        other = lax.rem(chip + i, CHIPS)
        return remote(mz, m2.at[chip], ms.at[1], mr.at[1], (other * NC + c, y))()

    everyone = bulk(m2.at[pl.ds(0, CHIPS - 1)], ms.at[1], mr.at[1])
    with jax.named_scope("far_send"):
        for i in range(CHIPS // 2, CHIPS // 2 + CHIPS - 1):
            far(1 + i % (CHIPS - 1)).start()
    with jax.named_scope("drain"):
        bulk(ft3.at[pl.ds(0, CHIPS - 1)], fs_sem.at[0], fr_sem.at[0]).wait_send()
        bulk(bb.at[:, :, 2], ps_sem.at[0], pr_sem.at[0]).wait_send()
        sent = pl.ds(1, NZ - 1)
        for n, (t1, t2, td) in enumerate([(ta1, ta2, tda), (tb1, tb2, tdb)]):
            bulk(t1.at[sent], s1.at[n], r1.at[0, 0]).wait_send()
            bulk(t2.at[sent], s1.at[2 + n], r1.at[0, 0]).wait_send()
            bulk(td.at[sent, pl.ds(0, NX - 1)], ds.at[n], dr.at[0, 0]).wait_send()
        bulk(sm.at[pl.ds(0, NZ - 1)], zs.at[0], zr.at[0]).wait_send()
        near.wait_send()
        for copy in raw_copies():
            copy().wait_send()

    with jax.named_scope("far_wait"):
        everyone.wait_recv()
    top_out[...] = jnp.max(m2[...], axis=0)
    everyone.wait_send()
    save.wait()


def finish(inten, top, out, peak):
    peak[...] = top[...]
    out[...] = inten[...] / (top[...] + 1.0)


def body(currents, leaf_basis, leaf_box, box_count, merge_factor, angle_factor):
    turned = jnp.transpose(merge_factor, (0, 2, 1)).reshape(2 * LR, NX * GX)

    vm = pltpu.VMEM
    dma = pltpu.SemaphoreType.DMA
    anyspace = pl.BlockSpec(memory_space=pl.ANY)
    invm = pl.BlockSpec(memory_space=pltpu.VMEM)
    shapes = (
        jax.ShapeDtypeStruct((A, EQ), F32),
        jax.ShapeDtypeStruct((1, EQ), F32),
    )
    inten, top = pl.pallas_call(
        kernel,
        out_shape=shapes,
        in_specs=[anyspace] * 6,
        out_specs=(anyspace, invm),
        scratch_shapes=[
            pltpu.SMEM((LEAF,), jnp.int32),
            vm((1, S_DEV), jnp.int32),
            vm((A, EQ), F32),
            vm((S_DEV, 2 * NE), BF),
            vm((2, R, S_DEV), BF),
            vm((2 * LR, NX * GX), BF),
            vm((A, 2, NX * GX), BF),
            vm((NX * GX, 2 * A), BF),
            vm((2 * LR, S_DEV), BF),
            vm((NX * GX, 2 * LR), BF),
            vm((2 * LR, 2 * NE), BF),
            vm((NZ, NX, 3, R, 2 * NE), BF),
            vm((CHIPS, NC * R, 2 * A), BF),
            vm((NZ, NX, NY, AR, EQ), F32),
            vm((NZ, NY, NX, BR, EQ), F32),
            vm((NZ, 4, AR, EQ), BF),
            vm((NZ, 4, BR, EQ), BF),
            vm((NZ, 2, 4, AR, EQ), BF),
            vm((NZ, 2, 4, BR, EQ), BF),
            vm((NZ, 2, 2, AR, EQ), BF),
            vm((NZ, 2, 2, BR, EQ), BF),
            vm((NZ, 2, 4, AR, EQ), BF),
            vm((NZ, 2, 4, BR, EQ), BF),
            vm((NZ, NY, AR, EQ), F32),
            vm((NZ, NX, BR, EQ), F32),
            vm((NZ, 2 * A, EQ), BF),
            vm((NZ, 2 * A, EQ), BF),
            vm((NX, NY, AR, EQ), BF),
            vm((NY, NX, BR, EQ), BF),
            vm((NX, NY, AR, EQ), BF),
            vm((NY, NX, BR, EQ), BF),
            vm((NZ, NY, AR, EQ), BF),
            vm((NZ, NX, BR, EQ), BF),
            vm((NZ, NY, AR, EQ), BF),
            vm((NZ, NX, BR, EQ), BF),
            vm((1, EQ), F32),
            vm((2, 1, EQ), F32),
            vm((1, EQ), F32),
            vm((CHIPS, 1, EQ), F32),
            dma((7,)),
            dma((1,)),
            dma((NZ,)),
            dma((1,)),
            dma((NZ,)),
            dma((4,)),
            dma((NZ, 4)),
            dma((1,)),
            dma((1,)),
            dma((2,)),
            dma((NZ, 2)),
            dma((2,)),
            dma((2,)),
            dma((2,)),
            dma((2,)),
        ],
        compiler_params=pltpu.CompilerParams(
            collective_id=0, has_side_effects=True, vmem_limit_bytes=62 * 1024 * 1024
        ),
    )(
        box_count,
        leaf_box.reshape(1, S_DEV),
        currents,
        leaf_basis,
        turned,
        angle_factor,
    )
    normalized, peak = pl.pallas_call(
        finish,
        out_shape=shapes,
        in_specs=[invm, invm],
        out_specs=(invm, invm),
    )(inten, top)
    return normalized, peak.reshape(EQ)


def solution(mesh):
    in_specs = (
        P(("src", "grp"), None),
        P(None, None, ("src", "grp")),
        P(("src", "grp")),
        P(("src", "grp")),
        P(None, None, ("src", "grp")),
        P("src", None, None, None),
    )
    out_specs = (P("src", "grp"), P("grp"))
    return jax.shard_map(body, mesh=mesh, in_specs=in_specs, out_specs=out_specs, check_vma=False)
```
